256 devices in a mesh: mem: 4 (over x_lo, core), ty: 8 (over x_hi, y), tx: 8 (over z).
Axes of the slice: x: 4 (x_hi: 2, x_lo: 2; x = x_hi * 2 + x_lo), y: 4, z: 8, core: 2. Of those that a mesh axis runs over, the one named last changes fastest.
Arguments:
- pressure: float32 [8, 50, 256, 1024], P('mem', None, 'ty', 'tx'), may hold values from -6 to 6
- east_wind: float32 [8, 50, 256, 1024], P('mem', None, 'ty', 'tx'), may hold values from -6 to 6
- north_wind: float32 [8, 50, 256, 1024], P('mem', None, 'ty', 'tx'), may hold values from -6 to 6
- vertical_wind: float32 [8, 49, 256, 1024], P('mem', None, 'ty', 'tx'), may hold values from -6 to 6
- sound_squared: float32 [50, 256, 1024], P(None, 'ty', 'tx'), may hold values from 0.5 to 2
- thickness: float32 [50], replicated, may hold values from 0.05 to 0.5
- owner_map: int32 [64], replicated, may hold values from 0 to 63, each once
Outputs:
- analysis: float32 [8, 8, 6, 32, 128], P('ty', 'tx', None, 'mem')
The draws below stay inside these ranges and needn't reach their ends.
Inputs may be any that keep to these rules, and one draw needn't show every extreme that they name: `owner_map`: every tile index appears exactly once.
All inputs are finite; a program needn't handle non-finite values.
Results may differ from the reference program's by a relative error of at most 0.0001.
Values sent between devices are 32-bit elements; how exact they have to be, the bound alone decides.
A program may use at most 128 MiB of HBM per device.

```python
import math
import jax
import jax.numpy as jnp
from jax import lax

CY = 32
CX = 128
NZ = 50
SUBSTEPS = 2
MEMBERS = 8
NY = 256
NX = 1024
WLEVELS = 49
TILES = 64
N_TY = 8
N_TX = 8


def levels(stream_key, dims, split, smallest, largest):
    def one(axis_at, parts):
        draws = jax.random.uniform(jax.random.fold_in(jax.random.fold_in(stream_key, 6), axis_at), (parts,), jnp.float32, smallest / len(split), largest / len(split))
        return jnp.repeat(jnp.exp(draws), dims[axis_at] // parts).reshape((-1,) + (1,) * (len(dims) - axis_at - 1))

    loudness = one(*split[0])
    for cut in split[1:]:
        loudness = loudness * one(*cut)
    return loudness


def noise(rng, shape, scale, most, pieces=(), held_as=jnp.bfloat16):
    array = jax.random.normal(rng, shape, jnp.float32) * scale
    if len(pieces) > 0:
        array = levels(rng, shape, pieces, -0.22, 0.18) * array
    return jnp.clip(array, min=-most, max=most).astype(held_as)


def setup_inputs(seed: int = 0) -> dict:
    key_list = jax.random.split(jax.random.key(seed), 8)
    return {
        "pressure": noise(key_list[0], (MEMBERS, NZ, NY, NX), 1.0, 6.0, ((0, 4), (2, 8), (3, 8)), jnp.float32),
        "east_wind": noise(key_list[1], (MEMBERS, NZ, NY, NX), 1.0, 6.0, ((0, 4), (2, 8), (3, 8)), jnp.float32),
        "north_wind": noise(key_list[2], (MEMBERS, NZ, NY, NX), 1.0, 6.0, ((0, 4), (2, 8), (3, 8)), jnp.float32),
        "vertical_wind": noise(key_list[3], (MEMBERS, WLEVELS, NY, NX), 1.0, 6.0, ((0, 4), (2, 8), (3, 8)), jnp.float32),
        "sound_squared": jnp.clip(jnp.exp(math.log(2.0) - 1.3862944 * jax.random.uniform(key_list[4], (NZ, NY, NX), jnp.float32) ** levels(key_list[4], (NZ, NY, NX), ((1, 8), (2, 8)), -0.2, 0.2)), 0.5, 2.0),
        "thickness": jnp.clip(jnp.exp(jax.random.uniform(key_list[5], (NZ,), jnp.float32, math.log(0.05), math.log(0.5))), 0.05, 0.5),
        "owner_map": jax.random.permutation(key_list[6], TILES).astype(jnp.int32),
    }


horiz_ratio = 0.35
vert_ratio = 1.5


def column_solve(coeff, rhs_list):
    count = len(rhs_list)
    factors = []
    values = []
    pivot = 1.0 + coeff[1] + coeff[0]
    values.append(rhs_list[0] / pivot)
    factors.append(-coeff[1] / pivot)
    for position in range(1, count):
        pivot = (1.0 + coeff[position + 1] + coeff[position]) + coeff[position] * factors[position - 1]
        values.append((rhs_list[position] + coeff[position] * values[position - 1]) / pivot)
        factors.append(-coeff[position + 1] / pivot)
    solved = [values[count - 1]]
    for position in range(count - 2, -1, -1):
        solved.insert(0, values[position] - factors[position] * solved[0])
    return solved


def member_run(pressure, east_wind, north_wind, vertical_wind, sound_squared, thickness):
    coeff_field = vert_ratio * vert_ratio * sound_squared
    coeff = [coeff_field[level] for level in range(NZ)]
    for substep in range(SUBSTEPS):
        east_wind = east_wind - horiz_ratio * (pressure - jnp.roll(pressure, 1, axis=2))
        north_wind = north_wind - horiz_ratio * (pressure - jnp.roll(pressure, 1, axis=1))
        divergence = (jnp.roll(east_wind, -1, axis=2) - east_wind) + (jnp.roll(north_wind, -1, axis=1) - north_wind)
        partial_value = pressure - horiz_ratio * sound_squared * divergence
        rhs_list = [vertical_wind[level] - vert_ratio * (partial_value[level + 1] - partial_value[level]) for level in range(NZ - 1)]
        vertical_wind = jnp.stack(column_solve(coeff, rhs_list), axis=0)
        zero_layer = jnp.zeros_like(partial_value[:1])
        padded = jnp.concatenate([zero_layer, vertical_wind, zero_layer], axis=0)
        pressure = partial_value - vert_ratio * sound_squared * (padded[1:] - padded[:-1])
    mass = jnp.einsum('k,kyx->yx', thickness, pressure, precision=lax.Precision.HIGHEST)
    east_total = jnp.einsum('k,kyx->yx', thickness, east_wind, precision=lax.Precision.HIGHEST)
    north_total = jnp.einsum('k,kyx->yx', thickness, north_wind, precision=lax.Precision.HIGHEST)
    return jnp.stack([mass, east_total, north_total], axis=0)


def reference(pressure, east_wind, north_wind, vertical_wind, sound_squared, thickness, owner_map):
    def one_member(fields):
        return member_run(fields[0], fields[1], fields[2], fields[3], sound_squared, thickness)

    integrals = lax.map(one_member, (pressure, east_wind, north_wind, vertical_wind))
    mean = jnp.sum(integrals, axis=0) / MEMBERS
    variance = jnp.sum((integrals - mean) ** 2, axis=0) / (MEMBERS - 1)
    stats = jnp.concatenate([mean, variance], axis=0)
    tiled = stats.reshape(6, N_TY, CY, N_TX, CX).transpose(1, 3, 0, 2, 4).reshape(N_TY * N_TX, 6, CY, CX)
    placed = jnp.zeros_like(tiled).at[owner_map.astype(jnp.int32)].set(tiled)
    return placed.reshape(N_TY, N_TX, 6, CY, CX)
```

```python
import functools

import jax
import jax.numpy as jnp
from jax import lax
from jax.experimental import pallas as pl
from jax.experimental.pallas import tpu as pltpu
from jax.sharding import PartitionSpec as P

HR = 0.35
VR = 1.5
PAD = 8
MESH = pl.DeviceIdType.MESH


def kernel(dims, thick, owner, p_h, ew_h, nw_h, w_h, ss_h, out_ref, *scratch):
    NM, NR, NC, NZ, CY, CX, U = dims
    (
        p_v, ew_v, nw_v, w_v, ss_v, part_v, ew1_v, nw1_v, v_v,
        rp_v, g_v, f_v, lam_v, gg_v, h_v, hw_v, he_v,
        sp_e, sq_w, srow_p, srow_q, sh_e, sh_w, shrow_n, shrow_s,
        rp_w, rq_e, rrow_p, rrow_q, rh_w, rh_e, rhrow_s, rhrow_n,
        acc_v, i_send, i_recv, ce_send, cw_send, ce_recv, cw_recv,
        rn_send, rs_send, rs_recv, rn_recv, gath, send2, recv2,
        ld_sem, hs_sem, hr_sem, is_sem, ir_sem, ces_sem, cer_sem, cws_sem, cwr_sem,
        rns_sem, rsr_sem, rss_sem, rnr_sem, gs_sem, gr_sem, a_s_sem, a_r_sem,
    ) = scratch
    Q = CY // NM
    m = lax.axis_index("mem")
    r = lax.axis_index("ty")
    c = lax.axis_index("tx")

    def mm(d):
        return lax.rem(m + d, NM)

    def rr(d):
        return lax.rem(r + d + NR, NR)

    def cc(d):
        return lax.rem(c + d + NC, NC)

    loads = [
        pltpu.make_async_copy(p_h, p_v.at[:, :, pl.ds(PAD, CY), :], ld_sem.at[0]),
        pltpu.make_async_copy(ew_h, ew_v, ld_sem.at[1]),
        pltpu.make_async_copy(nw_h, nw_v.at[:, :, pl.ds(PAD, CY), :], ld_sem.at[2]),
        pltpu.make_async_copy(ss_h, ss_v, ld_sem.at[3]),
        pltpu.make_async_copy(w_h, w_v.at[:, pl.ds(1, NZ - 1), :, :], ld_sem.at[4]),
    ]
    for ld in loads:
        ld.start()

    barrier = pltpu.get_barrier_semaphore()
    peers = [(m, r, cc(d)) for d in range(1, NC)]
    peers += [(m, rr(d), c) for d in range(1, NR)]
    peers += [(mm(d), r, c) for d in range(1, NM)]
    peers += [(mm(d), r, cc(s)) for d in range(1, NM) for s in (1, -1)]
    peers += [(mm(d), rr(s), c) for d in range(1, NM) for s in (1, -1)]
    for peer in peers:
        pl.semaphore_signal(barrier, inc=1, device_id=peer, device_id_type=MESH)

    sends = []

    def send(src, dst, ssem, rsem, dev):
        copy = pltpu.make_async_remote_copy(
            src_ref=src, dst_ref=dst, send_sem=ssem, recv_sem=rsem,
            device_id=dev, device_id_type=MESH,
        )
        copy.start()
        sends.append(copy)
        return copy

    east, west = (m, r, cc(1)), (m, r, cc(-1))
    north, south = (m, rr(1), c), (m, rr(-1), c)
    lane = lax.broadcasted_iota(jnp.int32, (CY, CX), 1)
    row = lax.broadcasted_iota(jnp.int32, (CY, CX), 0)
    own = pl.ds(PAD, CY)

    def blocked(body, init):
        def step(b, carry):
            for j in range(U):
                carry = body(b * U + j, carry)
            return carry

        return lax.fori_loop(0, NZ // U, step, init)

    loads[0].wait()
    loads[1].wait()
    loads[2].wait()

    def pack(k, carry):
        cp, cq = carry
        for a in range(2):
            l = a * NZ + k
            p = p_v[a, k, own, :]
            q = ew_v[a, k] - HR * p
            cp = jnp.where(lane == l, pltpu.roll(p, l + 1, 1), cp)
            cq = jnp.where(lane == l, pltpu.roll(q, l, 1), cq)
            srow_p[a, pl.ds(k, 1), :] = p_v[a, k, pl.ds(PAD + CY - 1, 1), :]
            srow_q[a, pl.ds(k, 1), :] = (
                nw_v[a, k, pl.ds(PAD, 1), :] - HR * p_v[a, k, pl.ds(PAD, 1), :]
            )
        return cp, cq

    zero = jnp.zeros((CY, CX), jnp.float32)
    cp, cq = blocked(pack, (zero, zero))
    sp_e[...] = cp
    sq_w[...] = cq

    pl.semaphore_wait(barrier, len(peers))
    halo = [
        send(srow_p, rrow_p, hs_sem.at[0], hr_sem.at[0], north),
        send(srow_q, rrow_q, hs_sem.at[1], hr_sem.at[1], south),
        send(sp_e, rp_w, hs_sem.at[2], hr_sem.at[2], east),
        send(sq_w, rq_e, hs_sem.at[3], hr_sem.at[3], west),
    ]

    loads[3].wait()

    def factor(k, carry):
        b_below, rp_below, ts_below, lv = carry
        ss = ss_v[k]
        b = (VR * VR) * ss
        pivot = (1.0 + b + b_below) - b_below * (b_below * rp_below)
        inner = jnp.where(k > 0, 1.0, 0.0)
        rp = inner / pivot
        g = b_below * rp
        ts = thick[k] * ss
        lv = (VR * (ts - ts_below)) * rp + g * lv
        rp_v[k] = rp
        g_v[k] = g
        f_v[k] = b * rp
        lam_v[k] = lv
        return b, rp, ts, lv

    blocked(factor, (zero, zero, zero, zero))

    def adjoint(i, carry):
        lam_up, he, hw = carry
        k = NZ - 1 - i
        lam = lam_v[k] + f_v[k] * lam_up
        gg = thick[k] + VR * (lam_up - lam)
        h = gg * ss_v[k]
        lam_v[k] = lam
        gg_v[k] = gg
        h_v[k, own, :] = h
        he = jnp.where(lane == k, pltpu.roll(h, k + 1, 1), he)
        hw = jnp.where(lane == k, pltpu.roll(h, k, 1), hw)
        return lam, he, hw

    _, he, hw = blocked(adjoint, (zero, zero, zero))
    sh_e[...] = he
    sh_w[...] = hw

    def hrows(k, carry):
        shrow_n[pl.ds(k, 1), :] = h_v[k, pl.ds(PAD + CY - 1, 1), :]
        shrow_s[pl.ds(k, 1), :] = h_v[k, pl.ds(PAD, 1), :]
        return carry

    blocked(hrows, 0)
    halo += [
        send(sh_e, rh_w, hs_sem.at[4], hr_sem.at[4], east),
        send(sh_w, rh_e, hs_sem.at[5], hr_sem.at[5], west),
        send(shrow_n, rhrow_s, hs_sem.at[6], hr_sem.at[6], north),
        send(shrow_s, rhrow_n, hs_sem.at[7], hr_sem.at[7], south),
    ]

    def find(t, got):
        o = owner[t]
        return tuple(
            jnp.where(o == rr(d) * NC + c, t, got[d]) for d in range(NR)
        )

    source = lax.fori_loop(0, NR * NC, find, tuple(jnp.int32(0) for _ in range(NR)))

    w_v[:, pl.ds(0, 1), :, :] = jnp.zeros((2, 1, CY, CX), jnp.float32)
    loads[4].wait()
    for copy in halo[:4]:
        copy.wait_recv()

    def put_rows(k, carry):
        for a in range(2):
            p_v[a, k, pl.ds(PAD - 1, 1), :] = rrow_p[a, pl.ds(k, 1), :]
            p_v[a, k, pl.ds(PAD + CY, 1), :] = jnp.zeros((1, CX), jnp.float32)
            nw_v[a, k, pl.ds(PAD + CY, 1), :] = rrow_q[a, pl.ds(k, 1), :]
        return carry

    blocked(put_rows, 0)
    p_west = rp_w[...]
    q_east = rq_e[...]

    def forward(k, carry):
        out = []
        ss = ss_v[k]
        for a in range(2):
            part_below, v = carry[a]
            l = a * NZ + k
            p = p_v[a, k, own, :]
            ew = ew_v[a, k]
            hp = HR * p
            pw = jnp.where(lane == 0, pltpu.roll(p_west, 2 * CX - l, 1), pltpu.roll(p, 1, 1))
            qe = jnp.where(
                lane == CX - 1,
                pltpu.roll(q_east, 2 * CX - 1 - l, 1),
                pltpu.roll(ew - hp, CX - 1, 1),
            )
            ew1 = ew - HR * (p - pw)
            nw1 = nw_v[a, k, own, :] - HR * (p - p_v[a, k, pl.ds(PAD - 1, CY), :])
            nn = nw_v[a, k, pl.ds(PAD + 1, CY), :] - HR * p_v[a, k, pl.ds(PAD + 1, CY), :] + hp
            div = (qe + hp - ew1) + (nn - nw1)
            part = p - (HR * ss) * div
            v = (w_v[a, k] - VR * (part - part_below)) * rp_v[k] + g_v[k] * v
            part_v[a, k] = part
            ew1_v[a, k] = ew1
            nw1_v[a, k] = nw1
            v_v[a, k] = v
            out.append((part, v))
        return tuple(out)

    blocked(forward, ((zero, zero), (zero, zero)))

    for copy in halo[4:]:
        copy.wait_recv()
    h_west = rh_w[...]
    h_east = rh_e[...]

    def shift_h(k, carry):
        h_v[k, pl.ds(PAD - 1, 1), :] = rhrow_s[pl.ds(k, 1), :]
        h_v[k, pl.ds(PAD + CY, 1), :] = rhrow_n[pl.ds(k, 1), :]
        h = h_v[k, own, :]
        hw_v[k] = jnp.where(lane == 0, pltpu.roll(h_west, CX - k, 1), pltpu.roll(h, 1, 1))
        he_v[k] = jnp.where(
            lane == CX - 1, pltpu.roll(h_east, CX - 1 - k, 1), pltpu.roll(h, CX - 1, 1)
        )
        return carry

    blocked(shift_h, 0)

    for b in range(CY // 8):
        rows = pl.ds(8 * b, 8)
        small = jnp.zeros((8, CX), jnp.float32)

        def backward(i, carry, rows=rows, b=b):
            k = NZ - 1 - i
            f = f_v[k, rows, :]
            lam = lam_v[k, rows, :]
            gg = gg_v[k, rows, :]
            vs = VR * ss_v[k, rows, :]
            h = h_v[k, pl.ds(PAD + 8 * b, 8), :]
            hs = h_v[k, pl.ds(PAD - 1 + 8 * b, 8), :]
            hn = h_v[k, pl.ds(PAD + 1 + 8 * b, 8), :]
            hwk = hw_v[k, rows, :]
            hek = he_v[k, rows, :]
            t = thick[k]
            out = []
            for a in range(2):
                w_up, s = carry[a]
                w = v_v[a, k, rows, :] + f * w_up
                p1 = part_v[a, k, rows, :] - vs * (w_up - w)
                ew1 = ew1_v[a, k, rows, :]
                nw1 = nw1_v[a, k, rows, :]
                hp = HR * p1
                re = hp - ew1
                rn = hp - nw1
                s = (
                    s[0] + (gg * p1 + lam * w),
                    s[1] + h * ((re + rn) + (hp + hp)),
                    s[2] + hwk * re,
                    s[3] + hek * hp,
                    s[4] + hs * rn,
                    s[5] + hn * hp,
                    s[6] + t * p1,
                    s[7] + t * ew1,
                    s[8] + t * nw1,
                )
                out.append((w, s))
            return tuple(out)

        init = tuple((small, (small,) * 9) for _ in range(2))
        done = blocked(backward, init)
        for a in range(2):
            s = done[a][1]
            acc_v[0, a, rows, :] = s[0] - HR * s[1]
            for j in range(2, 6):
                acc_v[j - 1, a, rows, :] = HR * s[j]
            acc_v[5, a, rows, :] = HR * s[6]
            acc_v[6, a, rows, :] = s[7]
            acc_v[7, a, rows, :] = s[8]

    to_e, to_w = zero, zero
    rn_send[...] = jnp.zeros_like(rn_send)
    rs_send[...] = jnp.zeros_like(rs_send)
    for a in range(2):
        base, xe, xw, xn, xs, hp, e1, n1 = (acc_v[j, a] for j in range(8))
        mass = (
            base
            + jnp.where(lane == CX - 1, 0.0, pltpu.roll(xe, CX - 1, 1))
            + jnp.where(lane == 0, 0.0, pltpu.roll(xw, 1, 1))
            + jnp.where(row == CY - 1, 0.0, pltpu.roll(xn, CY - 1, 0))
            + jnp.where(row == 0, 0.0, pltpu.roll(xs, 1, 0))
        )
        e2 = e1 - (hp - jnp.where(lane == 0, 0.0, pltpu.roll(hp, 1, 1)))
        n2 = n1 - (hp - jnp.where(row == 0, 0.0, pltpu.roll(hp, 1, 0)))
        for q in range(NM):
            i_send[q, 3 * a] = mass[q * Q : (q + 1) * Q]
            i_send[q, 3 * a + 1] = e2[q * Q : (q + 1) * Q]
            i_send[q, 3 * a + 2] = n2[q * Q : (q + 1) * Q]
        to_e = jnp.where(lane == a, pltpu.roll(xw, a + 1, 1), to_e)
        to_e = jnp.where(lane == 2 + a, pltpu.roll(hp, a + 3, 1), to_e)
        to_w = jnp.where(lane == a, pltpu.roll(xe, a, 1) if a else xe, to_w)
        rn_send[a : a + 1, :] = xs[CY - 1 : CY]
        rn_send[2 + a : 3 + a, :] = hp[CY - 1 : CY]
        rs_send[a : a + 1, :] = xn[0:1]
    for q in range(NM):
        ce_send[q] = to_e[q * Q : (q + 1) * Q]
        cw_send[q] = to_w[q * Q : (q + 1) * Q]

    send(rn_send, rs_recv.at[m], rns_sem.at[0], rsr_sem.at[m], (0, rr(1), c))
    send(rs_send, rn_recv.at[m], rss_sem.at[0], rnr_sem.at[m], (NM - 1, rr(-1), c))
    for d in range(NM):
        q = mm(d)
        send(ce_send.at[q], ce_recv.at[m], ces_sem.at[q], cer_sem.at[m], (q, r, cc(1)))
        send(cw_send.at[q], cw_recv.at[m], cws_sem.at[q], cwr_sem.at[m], (q, r, cc(-1)))
    for d in range(1, NM):
        q = mm(d)
        send(i_send.at[q], i_recv.at[m], is_sem.at[q], ir_sem.at[m], (q, r, c))
    i_recv[m] = i_send[m]

    def arrived(ref, sem, slot):
        pltpu.make_async_copy(ref.at[slot], ref.at[slot], sem.at[slot]).wait()

    for d in range(1, NM):
        arrived(i_recv, ir_sem, mm(d))
    for d in range(NM):
        arrived(ce_recv, cer_sem, mm(d))
        arrived(cw_recv, cwr_sem, mm(d))

    @pl.when(m == 0)
    def _():
        for d in range(NM):
            arrived(rs_recv, rsr_sem, mm(d))
        for s in range(NM):
            for a in range(2):
                i_recv[s, 3 * a, 0:1, :] += rs_recv[s, a : a + 1, :]
                i_recv[s, 3 * a + 2, 0:1, :] += rs_recv[s, 2 + a : 3 + a, :]

    @pl.when(m == NM - 1)
    def _():
        for d in range(NM):
            arrived(rn_recv, rnr_sem, mm(d))
        for s in range(NM):
            for a in range(2):
                i_recv[s, 3 * a, Q - 1 : Q, :] += rn_recv[s, a : a + 1, :]

    members = 2 * NM
    lane8 = lax.broadcasted_iota(jnp.int32, (Q, CX), 1)
    fields = ([], [], [])
    for s in range(NM):
        ce = ce_recv[s]
        cw = cw_recv[s]
        for a in range(2):
            mass = i_recv[s, 3 * a]
            mass += jnp.where(lane8 == 0, pltpu.roll(ce, CX - a, 1) if a else ce, 0.0)
            mass += jnp.where(lane8 == CX - 1, pltpu.roll(cw, CX - 1 - a, 1), 0.0)
            e2 = i_recv[s, 3 * a + 1]
            e2 += jnp.where(lane8 == 0, pltpu.roll(ce, CX - 2 - a, 1), 0.0)
            fields[0].append(mass)
            fields[1].append(e2)
            fields[2].append(i_recv[s, 3 * a + 2])
    for j in range(3):
        mean = sum(fields[j][1:], fields[j][0]) * (1.0 / members)
        devs = [(x - mean) * (x - mean) for x in fields[j]]
        gath[c, j] = mean
        gath[c, 3 + j] = sum(devs[1:], devs[0]) * (1.0 / (members - 1))

    for d in sorted(range(1, NC), key=lambda d: -min(d, NC - d)):
        send(gath.at[c], gath.at[c], gs_sem.at[d], gr_sem.at[c], (m, r, cc(d)))
    for d in range(1, NC):
        arrived(gath, gr_sem, cc(d))
    for d in sorted(range(1, NR), key=lambda d: -min(d, NR - d)):
        send2[d] = gath[lax.rem(source[d], NC)]
        send(send2.at[d], recv2.at[r], a_s_sem.at[d], a_r_sem.at[r], (m, rr(d), c))
    recv2[r] = gath[lax.rem(source[0], NC)]
    for d in range(1, NR):
        arrived(recv2, a_r_sem, rr(d))
    out_ref[0, 0] = recv2[source[0] // NC]
    for copy in sends:
        copy.wait_send()


def local(dims, pressure, east_wind, north_wind, vertical_wind, sound_squared, thickness, owner_map):
    NM, NR, NC, NZ, CY, CX, U = dims
    Q = CY // NM
    f32 = jnp.float32
    V = pltpu.VMEM
    D = pltpu.SemaphoreType.DMA
    rows = CY + 2 * PAD
    two = (2, NZ, CY, CX)
    one = (NZ, CY, CX)
    tile = (CY, CX)
    scratch = [
        V((2, NZ, rows, CX), f32), V(two, f32), V((2, NZ, rows, CX), f32), V(two, f32), V(one, f32),
        V(two, f32), V(two, f32), V(two, f32), V(two, f32),
        V(one, f32), V(one, f32), V(one, f32), V(one, f32), V(one, f32),
        V((NZ, rows, CX), f32), V(one, f32), V(one, f32),
        V(tile, f32), V(tile, f32), V((2, NZ, CX), f32), V((2, NZ, CX), f32),
        V(tile, f32), V(tile, f32), V((NZ, CX), f32), V((NZ, CX), f32),
        V(tile, f32), V(tile, f32), V((2, NZ, CX), f32), V((2, NZ, CX), f32),
        V(tile, f32), V(tile, f32), V((NZ, CX), f32), V((NZ, CX), f32),
        V((8, 2, CY, CX), f32), V((NM, 6, Q, CX), f32), V((NM, 6, Q, CX), f32),
        V((NM, Q, CX), f32), V((NM, Q, CX), f32), V((NM, Q, CX), f32), V((NM, Q, CX), f32),
        V((8, CX), f32), V((8, CX), f32), V((NM, 8, CX), f32), V((NM, 8, CX), f32),
        V((NC, 6, Q, CX), f32), V((NR, 6, Q, CX), f32), V((NR, 6, Q, CX), f32),
        D((5,)), D((8,)), D((8,)), D((NM,)), D((NM,)),
        D((NM,)), D((NM,)), D((NM,)), D((NM,)),
        D((1,)), D((NM,)), D((1,)), D((NM,)),
        D((NC,)), D((NC,)), D((NR,)), D((NR,)),
    ]
    smem = pl.BlockSpec(memory_space=pltpu.SMEM)
    hbm = pl.BlockSpec(memory_space=pl.ANY)
    return pl.pallas_call(
        functools.partial(kernel, dims),
        out_shape=jax.ShapeDtypeStruct((1, 1, 6, Q, CX), f32),
        in_specs=[smem, smem] + [hbm] * 5,
        out_specs=pl.BlockSpec(memory_space=pltpu.VMEM),
        scratch_shapes=scratch,
        compiler_params=pltpu.CompilerParams(
            collective_id=0, has_side_effects=True, vmem_limit_bytes=60000 * 1024
        ),
        name="substeps",
    )(thickness, owner_map, pressure, east_wind, north_wind, vertical_wind, sound_squared)


def solution(mesh):
    placed = (
        P("mem", None, "ty", "tx"),
        P("mem", None, "ty", "tx"),
        P("mem", None, "ty", "tx"),
        P("mem", None, "ty", "tx"),
        P(None, "ty", "tx"),
        P(),
        P(),
    )

    def step(*args):
        levels = args[0].shape[1]
        dims = (
            mesh.shape["mem"], mesh.shape["ty"], mesh.shape["tx"], levels,
            args[0].shape[2] , args[0].shape[3], 10 if levels % 10 == 0 else 1,
        )
        return local(dims, *args)

    return jax.shard_map(
        step,
        mesh=mesh,
        in_specs=placed,
        out_specs=P("ty", "tx", None, "mem", None),
        check_vma=False,
    )
```

```python
import functools

import jax
import jax.numpy as jnp
from jax import lax
from jax.experimental import pallas as pl
from jax.experimental.pallas import tpu as pltpu
from jax.sharding import PartitionSpec as P

HR = 0.35
VR = 1.5
PAD = 8
MESH = pl.DeviceIdType.MESH


def kernel(dims, thick_h, owner_h, p_h, ew_h, nw_h, w_h, ss_h, out_ref, *scratch):
    NM, NR, NC, NZ, CY, CX, U = dims
    (
        thick, owner,
        p_v, ew_v, nw_v, w_v, ss_v, part_v, ew1_v, nw1_v, v_v,
        rp_v, g_v, f_v, lam_v, gg_v, h_v, hw_v, he_v,
        z_send, srow_p, srow_q, zh_send, shrow_n, shrow_s,
        z_w, z_e, rrow_p, rrow_q, zh_w, zh_e, rhrow_s, rhrow_n,
        acc_v, i_send, i_recv, ce_send, cw_send, ce_recv, cw_recv,
        rn_send, rs_send, rs_recv, rn_recv,
        gath_a, gath_b, send_a, send_b, recv_a, recv_b,
        ld_sem, hs_sem, hr_sem, is_sem, ir_sem, ces_sem, cer_sem, cws_sem, cwr_sem,
        rns_sem, rsr_sem, rss_sem, rnr_sem,
        ga_s, ga_r, gb_s, gb_r, sa_s, sa_r, sb_s, sb_r,
    ) = scratch
    Q = CY // NM
    m = lax.axis_index("mem")
    r = lax.axis_index("ty")
    c = lax.axis_index("tx")

    def mm(d):
        return lax.rem(m + d, NM)

    def rr(d):
        return lax.rem(r + d + NR, NR)

    def cc(d):
        return lax.rem(c + d + NC, NC)

    own = pl.ds(PAD, CY)
    load_p = [pltpu.make_async_copy(p_h.at[a], p_v.at[a, :, own, :], ld_sem.at[a]) for a in range(2)]
    load_e = [pltpu.make_async_copy(ew_h.at[a], ew_v.at[a], ld_sem.at[2 + a]) for a in range(2)]
    load_n = pltpu.make_async_copy(nw_h, nw_v.at[:, :, own, :], ld_sem.at[4])
    load_s = pltpu.make_async_copy(ss_h, ss_v, ld_sem.at[5])
    load_w = pltpu.make_async_copy(w_h, w_v.at[:, pl.ds(1, NZ - 1), :, :], ld_sem.at[6])
    load_t = pltpu.make_async_copy(thick_h, thick, ld_sem.at[7])
    load_o = pltpu.make_async_copy(owner_h, owner, ld_sem.at[8])
    for ld in (load_p[0], load_e[0], load_p[1], load_e[1], load_n, load_s, load_t, load_w, load_o):
        ld.start()

    barrier = pltpu.get_barrier_semaphore()
    peers = [(m, r, cc(d)) for d in range(1, NC)]
    peers += [(m, rr(d), c) for d in range(1, NR)]
    peers += [(mm(d), r, c) for d in range(1, NM)]
    peers += [(mm(d), r, cc(s)) for d in range(1, NM) for s in (1, -1)]
    peers += [(mm(d), rr(s), c) for d in range(1, NM) for s in (1, -1)]
    for peer in peers:
        pl.semaphore_signal(barrier, inc=1, device_id=peer, device_id_type=MESH)

    sends = []

    def send(src, dst, ssem, rsem, dev):
        copy = pltpu.make_async_remote_copy(
            src_ref=src, dst_ref=dst, send_sem=ssem, recv_sem=rsem,
            device_id=dev, device_id_type=MESH,
        )
        copy.start()
        sends.append(copy)
        return copy

    def arrived(ref, sem, slot):
        pltpu.make_async_copy(ref.at[slot], ref.at[slot], sem.at[slot]).wait()

    east, west = (m, r, cc(1)), (m, r, cc(-1))
    north, south = (m, rr(1), c), (m, rr(-1), c)
    lane = lax.broadcasted_iota(jnp.int32, (CY, CX), 1)
    row = lax.broadcasted_iota(jnp.int32, (CY, CX), 0)
    lane8 = lax.broadcasted_iota(jnp.int32, (8, CX), 1)
    row8 = lax.broadcasted_iota(jnp.int32, (8, CX), 0)
    zero = jnp.zeros((CY, CX), jnp.float32)
    line = jnp.zeros((1, CX), jnp.float32)

    def blocked(body, init, u=U):
        if u >= NZ:
            for k in range(NZ):
                init = body(k, init)
            return init

        def step(b, carry):
            for j in range(u):
                carry = body(b * u + j, carry)
            return carry

        return lax.fori_loop(0, NZ // u, step, init)

    for a in range(2):
        load_p[a].wait()
        load_e[a].wait()

        def pack(k, z, a=a):
            p = p_v[a, k, own, :]
            edge = jnp.where(lane == CX - 1, p, ew_v[a, k] - HR * p)
            srow_p[a, pl.ds(k, 1), :] = p_v[a, k, pl.ds(PAD + CY - 1, 1), :]
            return jnp.where((lane >> 1) == k, pltpu.roll(edge, 2 * k + 1, 1), z)

        z_send[a] = blocked(pack, zero, NZ)

    load_n.wait()

    def pack_rows(k, carry):
        for a in range(2):
            srow_q[a, pl.ds(k, 1), :] = (
                nw_v[a, k, pl.ds(PAD, 1), :] - HR * p_v[a, k, pl.ds(PAD, 1), :]
            )
        return carry

    blocked(pack_rows, 0)

    pl.semaphore_wait(barrier, len(peers))
    halo = [
        send(srow_p, rrow_p, hs_sem.at[0], hr_sem.at[0], north),
        send(srow_q, rrow_q, hs_sem.at[1], hr_sem.at[1], south),
        send(z_send, z_w, hs_sem.at[2], hr_sem.at[2], east),
        send(z_send, z_e, hs_sem.at[3], hr_sem.at[3], west),
    ]

    load_s.wait()
    load_t.wait()

    def factor(k, carry):
        b_below, rp_below, ts_below, lv = carry
        ss = ss_v[k]
        b = (VR * VR) * ss
        pivot = (1.0 + b + b_below) - b_below * (b_below * rp_below)
        rp = jnp.where(k > 0, 1.0, 0.0) / pivot
        g = b_below * rp
        ts = thick[k] * ss
        lv = (VR * (ts - ts_below)) * rp + g * lv
        rp_v[k] = rp
        g_v[k] = g
        f_v[k] = b * rp
        lam_v[k] = lv
        return b, rp, ts, lv

    blocked(factor, (zero, zero, zero, zero))

    def adjoint(i, carry):
        lam_up, z = carry
        k = NZ - 1 - i
        lam = lam_v[k] + f_v[k] * lam_up
        gg = thick[k] + VR * (lam_up - lam)
        h = gg * ss_v[k]
        lam_v[k] = lam
        gg_v[k] = gg
        h_v[k, own, :] = h
        shrow_n[pl.ds(k, 1), :] = h[CY - 1 : CY]
        shrow_s[pl.ds(k, 1), :] = h[0:1]
        hw_v[k] = pltpu.roll(h, 1, 1)
        he_v[k] = pltpu.roll(h, CX - 1, 1)
        return lam, jnp.where((lane >> 1) == k, pltpu.roll(h, 2 * k + 1, 1), z)

    zh_send[...] = blocked(adjoint, (zero, zero))[1]
    halo += [
        send(zh_send, zh_w, hs_sem.at[4], hr_sem.at[4], east),
        send(zh_send, zh_e, hs_sem.at[5], hr_sem.at[5], west),
        send(shrow_n, rhrow_s, hs_sem.at[6], hr_sem.at[6], north),
        send(shrow_s, rhrow_n, hs_sem.at[7], hr_sem.at[7], south),
    ]

    def clear(k, carry):
        for a in range(2):
            p_v[a, k, pl.ds(PAD - 1, 1), :] = line
            p_v[a, k, pl.ds(PAD + CY, 1), :] = line
            nw_v[a, k, pl.ds(PAD + CY, 1), :] = line
        return carry

    blocked(clear, 0)

    def inner(k, carry):
        hs = HR * ss_v[k]
        for a in range(2):
            p = p_v[a, k, own, :]
            hp = HR * p
            q = ew_v[a, k] - hp
            ew1 = q + jnp.where(lane == 0, 0.0, pltpu.roll(hp, 1, 1))
            ee = hp + jnp.where(lane == CX - 1, 0.0, pltpu.roll(q, CX - 1, 1))
            nw1 = nw_v[a, k, own, :] - hp + HR * p_v[a, k, pl.ds(PAD - 1, CY), :]
            nn = nw_v[a, k, pl.ds(PAD + 1, CY), :] - HR * p_v[a, k, pl.ds(PAD + 1, CY), :] + hp
            part_v[a, k] = p - hs * ((ee - ew1) + (nn - nw1))
            ew1_v[a, k] = ew1
            nw1_v[a, k] = nw1
        return carry

    blocked(inner, 0)

    w_v[:, pl.ds(0, 1), :, :] = jnp.zeros((2, 1, CY, CX), jnp.float32)
    load_w.wait()
    halo[2].wait_recv()
    halo[3].wait_recv()

    even = (lane & 1) == 0
    for a in range(2):
        z_w[a] = jnp.where(even, z_w[a], pltpu.roll(z_e[a], CX - 2, 1))
    div_lane = jnp.where(lane8 == CX - 1, 1.0, jnp.where(lane8 == 0, -HR, 0.0))
    ew_lane = jnp.where(lane8 == 0, HR, 0.0)
    small = jnp.zeros((8, CX), jnp.float32)

    def forward(blocks):
        def body(k, carry):
            out = []
            for i, b in enumerate(blocks):
                rows = pl.ds(8 * b, 8)
                hs = HR * ss_v[k, rows, :]
                rp = rp_v[k, rows, :]
                g = g_v[k, rows, :]
                for a in range(2):
                    part_below, v = carry[2 * i + a]
                    edge = pltpu.roll(z_w[a, rows, :], 2 * CX - 2 * k, 1)
                    more = edge * div_lane
                    if b == 0:
                        below = jnp.where(row8 == 0, HR * rrow_p[a, pl.ds(k, 1), :], 0.0)
                        more = more - below
                        nw1_v[a, k, rows, :] += below
                    if b == CY // 8 - 1:
                        more = more + jnp.where(row8 == 7, rrow_q[a, pl.ds(k, 1), :], 0.0)
                    part = part_v[a, k, rows, :] - hs * more
                    v = (w_v[a, k, rows, :] - VR * (part - part_below)) * rp + g * v
                    part_v[a, k, rows, :] = part
                    ew1_v[a, k, rows, :] += edge * ew_lane
                    v_v[a, k, rows, :] = v
                    out.append((part, v))
            return tuple(out)

        blocked(body, ((small, small),) * (2 * len(blocks)))

    forward(tuple(range(1, CY // 8 - 1)))
    halo[0].wait_recv()
    halo[1].wait_recv()
    forward((0, CY // 8 - 1))

    for copy in halo[4:]:
        copy.wait_recv()

    def put_rows(k, carry):
        h_v[k, pl.ds(PAD - 1, 1), :] = rhrow_s[pl.ds(k, 1), :]
        h_v[k, pl.ds(PAD + CY, 1), :] = rhrow_n[pl.ds(k, 1), :]
        return carry

    blocked(put_rows, 0)
    zh_w[...] = jnp.where(even, zh_w[...], pltpu.roll(zh_e[...], CX - 2, 1))

    def backward(b):
        rows = pl.ds(8 * b, 8)

        def body(i, carry):
            k = NZ - 1 - i
            f = f_v[k, rows, :]
            lam = lam_v[k, rows, :]
            gg = gg_v[k, rows, :]
            vs = VR * ss_v[k, rows, :]
            h = h_v[k, pl.ds(PAD + 8 * b, 8), :]
            hs = h_v[k, pl.ds(PAD - 1 + 8 * b, 8), :]
            hn = h_v[k, pl.ds(PAD + 1 + 8 * b, 8), :]
            edge = pltpu.roll(zh_w[rows, :], 2 * CX - 2 * k, 1)
            hwk = jnp.where(lane8 == 0, edge, hw_v[k, rows, :])
            hek = jnp.where(lane8 == CX - 1, edge, he_v[k, rows, :])
            t = thick[k]
            out = []
            for a in range(2):
                w_up, s = carry[a]
                w = v_v[a, k, rows, :] + f * w_up
                p1 = part_v[a, k, rows, :] - vs * (w_up - w)
                ew1 = ew1_v[a, k, rows, :]
                nw1 = nw1_v[a, k, rows, :]
                hp = HR * p1
                re = hp - ew1
                rn = hp - nw1
                s = (
                    s[0] + (gg * p1 + lam * w),
                    s[1] + h * ((re + rn) + (hp + hp)),
                    s[2] + hwk * re,
                    s[3] + hek * hp,
                    s[4] + hs * rn,
                    s[5] + hn * hp,
                    s[6] + t * p1,
                    s[7] + t * ew1,
                    s[8] + t * nw1,
                )
                out.append((w, s))
            return tuple(out)

        done = blocked(body, ((small, (small,) * 9),) * 2)
        for a in range(2):
            s = done[a][1]
            acc_v[0, a, rows, :] = s[0] - HR * s[1]
            for j in range(2, 6):
                acc_v[j - 1, a, rows, :] = HR * s[j]
            acc_v[5, a, rows, :] = HR * s[6]
            acc_v[6, a, rows, :] = s[7]
            acc_v[7, a, rows, :] = s[8]

    backward(CY // 8 - 1)
    backward(0)

    rn_send[...] = jnp.zeros_like(rn_send)
    rs_send[...] = jnp.zeros_like(rs_send)
    last = pl.ds(CY - 1, 1)
    for a in range(2):
        rn_send[a : a + 1, :] = acc_v[4, a, last, :]
        rn_send[2 + a : 3 + a, :] = acc_v[5, a, last, :]
        rs_send[a : a + 1, :] = acc_v[3, a, pl.ds(0, 1), :]
    send(rn_send, rs_recv.at[m], rns_sem.at[0], rsr_sem.at[m], (0, rr(1), c))
    send(rs_send, rn_recv.at[m], rss_sem.at[0], rnr_sem.at[m], (NM - 1, rr(-1), c))

    for b in range(1, CY // 8 - 1):
        backward(b)

    to_e, to_w = zero, zero
    for a in range(2):
        base, xe, xw, xn, xs, hp, e1, n1 = (acc_v[j, a] for j in range(8))
        mass = (
            base
            + jnp.where(lane == CX - 1, 0.0, pltpu.roll(xe, CX - 1, 1))
            + jnp.where(lane == 0, 0.0, pltpu.roll(xw, 1, 1))
            + jnp.where(row == CY - 1, 0.0, pltpu.roll(xn, CY - 1, 0))
            + jnp.where(row == 0, 0.0, pltpu.roll(xs, 1, 0))
        )
        e2 = e1 - (hp - jnp.where(lane == 0, 0.0, pltpu.roll(hp, 1, 1)))
        n2 = n1 - (hp - jnp.where(row == 0, 0.0, pltpu.roll(hp, 1, 0)))
        for q in range(NM):
            i_send[q, 3 * a] = mass[q * Q : (q + 1) * Q]
            i_send[q, 3 * a + 1] = e2[q * Q : (q + 1) * Q]
            i_send[q, 3 * a + 2] = n2[q * Q : (q + 1) * Q]
        to_e = jnp.where(lane == a, pltpu.roll(xw, a + 1, 1), to_e)
        to_e = jnp.where(lane == 2 + a, pltpu.roll(hp, a + 3, 1), to_e)
        to_w = jnp.where(lane == a, pltpu.roll(xe, a, 1) if a else xe, to_w)
    for q in range(NM):
        ce_send[q] = to_e[q * Q : (q + 1) * Q]
        cw_send[q] = to_w[q * Q : (q + 1) * Q]

    for d in range(NM):
        q = mm(d)
        send(ce_send.at[q], ce_recv.at[m], ces_sem.at[q], cer_sem.at[m], (q, r, cc(1)))
        send(cw_send.at[q], cw_recv.at[m], cws_sem.at[q], cwr_sem.at[m], (q, r, cc(-1)))
    for d in range(1, NM):
        q = mm(d)
        send(i_send.at[q], i_recv.at[m], is_sem.at[q], ir_sem.at[m], (q, r, c))
    i_recv[m] = i_send[m]

    for d in range(1, NM):
        arrived(i_recv, ir_sem, mm(d))
    for d in range(NM):
        arrived(ce_recv, cer_sem, mm(d))
        arrived(cw_recv, cwr_sem, mm(d))

    @pl.when(m == 0)
    def _():
        for d in range(NM):
            arrived(rs_recv, rsr_sem, mm(d))
        for s in range(NM):
            for a in range(2):
                i_recv[s, 3 * a, 0:1, :] += rs_recv[s, a : a + 1, :]
                i_recv[s, 3 * a + 2, 0:1, :] += rs_recv[s, 2 + a : 3 + a, :]

    @pl.when(m == NM - 1)
    def _():
        for d in range(NM):
            arrived(rn_recv, rnr_sem, mm(d))
        for s in range(NM):
            for a in range(2):
                i_recv[s, 3 * a, Q - 1 : Q, :] += rn_recv[s, a : a + 1, :]

    members = 2 * NM
    fields = ([], [], [])
    for s in range(NM):
        ce = ce_recv[s]
        cw = cw_recv[s]
        for a in range(2):
            mass = i_recv[s, 3 * a]
            mass += jnp.where(lane8 == 0, pltpu.roll(ce, CX - a, 1) if a else ce, 0.0)
            mass += jnp.where(lane8 == CX - 1, pltpu.roll(cw, CX - 1 - a, 1), 0.0)
            e2 = i_recv[s, 3 * a + 1]
            e2 += jnp.where(lane8 == 0, pltpu.roll(ce, CX - 2 - a, 1), 0.0)
            fields[0].append(mass)
            fields[1].append(e2)
            fields[2].append(i_recv[s, 3 * a + 2])
    for j in range(3):
        mean = sum(fields[j][1:], fields[j][0]) * (1.0 / members)
        devs = [(x - mean) * (x - mean) for x in fields[j]]
        gath_a[c, j] = mean
        gath_b[r, j] = sum(devs[1:], devs[0]) * (1.0 / (members - 1))

    def far(n):
        return sorted(range(1, n), key=lambda d: -min(d, n - d))

    for d in far(NC):
        send(gath_a.at[c], gath_a.at[c], ga_s.at[d], ga_r.at[c], (m, r, cc(d)))
    for d in far(NR):
        send(gath_b.at[r], gath_b.at[r], gb_s.at[d], gb_r.at[r], (m, rr(d), c))

    load_o.wait()
    wanted = [rr(d) * NC + c for d in range(NR)] + [r * NC + cc(d) for d in range(1, NC)]

    def find(i, got):
        for j in range(8 if NR * NC % 8 == 0 else 1):
            t = i * (8 if NR * NC % 8 == 0 else 1) + j
            o = owner[t]
            got = tuple(jnp.where(o == w, t, g) for w, g in zip(wanted, got))
        return got

    steps = NR * NC // 8 if NR * NC % 8 == 0 else NR * NC
    source = lax.fori_loop(0, steps, find, tuple(jnp.int32(0) for _ in wanted))
    col_source, row_source = source[:NR], source[:1] + source[NR:]

    for d in range(1, NC):
        arrived(gath_a, ga_r, cc(d))
    for d in far(NR):
        send_a[d] = gath_a[lax.rem(col_source[d], NC)]
        send(send_a.at[d], recv_a.at[r], sa_s.at[d], sa_r.at[r], (m, rr(d), c))
    for d in range(1, NR):
        arrived(gath_b, gb_r, rr(d))
    for d in far(NC):
        send_b[d] = gath_b[row_source[d] // NC]
        send(send_b.at[d], recv_b.at[c], sb_s.at[d], sb_r.at[c], (m, r, cc(d)))
    recv_a[r] = gath_a[lax.rem(source[0], NC)]
    recv_b[c] = gath_b[source[0] // NC]
    for d in range(1, NR):
        arrived(recv_a, sa_r, rr(d))
    for d in range(1, NC):
        arrived(recv_b, sb_r, cc(d))
    out_ref[0, 0, 0:3] = recv_a[source[0] // NC]
    out_ref[0, 0, 3:6] = recv_b[lax.rem(source[0], NC)]
    for copy in sends:
        copy.wait_send()


def local(dims, pressure, east_wind, north_wind, vertical_wind, sound_squared, thickness, owner_map):
    NM, NR, NC, NZ, CY, CX, U = dims
    Q = CY // NM
    f32 = jnp.float32
    V = pltpu.VMEM
    D = pltpu.SemaphoreType.DMA
    rows = CY + 2 * PAD
    two = (2, NZ, CY, CX)
    one = (NZ, CY, CX)
    tile = (CY, CX)
    pair = (2, CY, CX)
    scratch = [
        pltpu.SMEM((NZ,), f32), pltpu.SMEM((NR * NC,), jnp.int32),
        V((2, NZ, rows, CX), f32), V(two, f32), V((2, NZ, rows, CX), f32), V(two, f32), V(one, f32),
        V(two, f32), V(two, f32), V(two, f32), V(two, f32),
        V(one, f32), V(one, f32), V(one, f32), V(one, f32), V(one, f32),
        V((NZ, rows, CX), f32), V(one, f32), V(one, f32),
        V(pair, f32), V((2, NZ, CX), f32), V((2, NZ, CX), f32),
        V(tile, f32), V((NZ, CX), f32), V((NZ, CX), f32),
        V(pair, f32), V(pair, f32), V((2, NZ, CX), f32), V((2, NZ, CX), f32),
        V(tile, f32), V(tile, f32), V((NZ, CX), f32), V((NZ, CX), f32),
        V((8, 2, CY, CX), f32), V((NM, 6, Q, CX), f32), V((NM, 6, Q, CX), f32),
        V((NM, Q, CX), f32), V((NM, Q, CX), f32), V((NM, Q, CX), f32), V((NM, Q, CX), f32),
        V((8, CX), f32), V((8, CX), f32), V((NM, 8, CX), f32), V((NM, 8, CX), f32),
        V((NC, 3, Q, CX), f32), V((NR, 3, Q, CX), f32),
        V((NR, 3, Q, CX), f32), V((NC, 3, Q, CX), f32),
        V((NR, 3, Q, CX), f32), V((NC, 3, Q, CX), f32),
        D((9,)), D((8,)), D((8,)), D((NM,)), D((NM,)),
        D((NM,)), D((NM,)), D((NM,)), D((NM,)),
        D((1,)), D((NM,)), D((1,)), D((NM,)),
        D((NC,)), D((NC,)), D((NR,)), D((NR,)), D((NR,)), D((NR,)), D((NC,)), D((NC,)),
    ]
    hbm = pl.BlockSpec(memory_space=pl.ANY)
    return pl.pallas_call(
        functools.partial(kernel, dims),
        out_shape=jax.ShapeDtypeStruct((1, 1, 6, Q, CX), f32),
        in_specs=[hbm] * 7,
        out_specs=pl.BlockSpec(memory_space=pltpu.VMEM),
        scratch_shapes=scratch,
        compiler_params=pltpu.CompilerParams(
            collective_id=0, has_side_effects=True, vmem_limit_bytes=60000 * 1024
        ),
        name="substeps",
    )(thickness, owner_map, pressure, east_wind, north_wind, vertical_wind, sound_squared)


def solution(mesh):
    placed = (
        P("mem", None, "ty", "tx"),
        P("mem", None, "ty", "tx"),
        P("mem", None, "ty", "tx"),
        P("mem", None, "ty", "tx"),
        P(None, "ty", "tx"),
        P(),
        P(),
    )

    def step(*args):
        levels = args[0].shape[1]
        dims = (
            mesh.shape["mem"], mesh.shape["ty"], mesh.shape["tx"], levels,
            args[0].shape[2] , args[0].shape[3], 25 if levels % 25 == 0 else 1,
        )
        return local(dims, *args)

    return jax.shard_map(
        step,
        mesh=mesh,
        in_specs=placed,
        out_specs=P("ty", "tx", None, "mem", None),
        check_vma=False,
    )
```

```python
import functools

import jax
import jax.numpy as jnp
from jax import lax
from jax.experimental import pallas as pl
from jax.experimental.pallas import tpu as pltpu
from jax.sharding import PartitionSpec as P

HR = 0.35
VR = 1.5
PAD = 8
MESH = pl.DeviceIdType.MESH


def kernel(dims, thick_h, owner_h, p_h, ew_h, nw_h, w_h, ss_h, out_ref, *scratch):
    NM, NR, NC, NZ, CY, CX, U = dims
    (
        thick, owner,
        p_v, ew_v, nw_v, w_v, ss_v, part_v, v_v,
        rp_v, g_v, f_v, lam_v, c_v, h_v, hw_v, he_v,
        z_send, srow_p, srow_q, row_p, zh_send, shrow_n, shrow_s, edge_p, edge_n, rrow_n,
        z_w, z_e, rrow_p, rrow_q, zh_w, zh_e, rhrow_s, rhrow_n,
        edge_h, sum_v, acc_v, i_send, i_recv, ce_send, cw_send, ce_recv, cw_recv,
        rn_send, rs_send, rs_recv, rn_recv,
        gath_a, gath_b, send_a, send_b, recv_a, recv_b,
        tok_sem, ld_sem, hs_sem, hr_sem, is_sem, ir_sem, ces_sem, cer_sem, cws_sem, cwr_sem,
        rns_sem, rsr_sem, rss_sem, rnr_sem,
        ga_s, ga_r, gb_s, gb_r, sa_s, sa_r, sb_s, sb_r,
    ) = scratch
    Q = CY // NM
    m = lax.axis_index("mem")
    r = lax.axis_index("ty")
    c = lax.axis_index("tx")

    def mm(d):
        return lax.rem(m + d, NM)

    def rr(d):
        return lax.rem(r + d + NR, NR)

    def cc(d):
        return lax.rem(c + d + NC, NC)

    own = pl.ds(PAD, CY)
    load_p = [pltpu.make_async_copy(p_h.at[a], p_v.at[a, :, own, :], ld_sem.at[a]) for a in range(2)]
    load_e = [pltpu.make_async_copy(ew_h.at[a], ew_v.at[a], ld_sem.at[2 + a]) for a in range(2)]
    load_n = pltpu.make_async_copy(nw_h, nw_v.at[:, :, own, :], ld_sem.at[4])
    load_s = pltpu.make_async_copy(ss_h, ss_v, ld_sem.at[5])
    load_w = pltpu.make_async_copy(w_h, w_v.at[:, pl.ds(1, NZ - 1), :, :], ld_sem.at[6])
    load_t = pltpu.make_async_copy(thick_h, thick, ld_sem.at[7])
    load_o = pltpu.make_async_copy(owner_h, owner, ld_sem.at[8])
    load_rows = [
        pltpu.make_async_copy(p_h.at[:, :, CY - 1, :], srow_p, ld_sem.at[9]),
        pltpu.make_async_copy(p_h.at[:, :, 0, :], row_p, ld_sem.at[10]),
        pltpu.make_async_copy(nw_h.at[:, :, 0, :], srow_q, ld_sem.at[11]),
    ]
    for ld in (*load_rows, load_p[0], load_e[0], load_p[1], load_e[1], load_s, load_t, load_n, load_w, load_o):
        ld.start()

    barrier = pltpu.get_barrier_semaphore()
    east, west = (m, r, cc(1)), (m, r, cc(-1))
    north, south = (m, rr(1), c), (m, rr(-1), c)
    around = (north, south, east, west)
    peers = [*around, *((mm(d), r, c) for d in range(1, NM))]
    for peer in peers:
        pl.semaphore_signal(barrier, inc=1, device_id=peer, device_id_type=MESH)

    sends = []

    def send(src, dst, ssem, rsem, dev):
        copy = pltpu.make_async_remote_copy(
            src_ref=src, dst_ref=dst, send_sem=ssem, recv_sem=rsem,
            device_id=dev, device_id_type=MESH,
        )
        copy.start()
        sends.append(copy)
        return copy

    def arrived(ref, sem, slot):
        pltpu.make_async_copy(ref.at[slot], ref.at[slot], sem.at[slot]).wait()

    def tell(sem):
        for peer in around:
            pl.semaphore_signal(sem, inc=1, device_id=peer, device_id_type=MESH)

    lane = lax.broadcasted_iota(jnp.int32, (CY, CX), 1)
    row = lax.broadcasted_iota(jnp.int32, (CY, CX), 0)
    lane8 = lax.broadcasted_iota(jnp.int32, (8, CX), 1)
    row8 = lax.broadcasted_iota(jnp.int32, (8, CX), 0)
    zero = jnp.zeros((CY, CX), jnp.float32)
    line = jnp.zeros((1, CX), jnp.float32)

    def blocked(body, init, u=U):
        if u >= NZ:
            for k in range(NZ):
                init = body(k, init)
            return init

        def step(b, carry):
            for j in range(u):
                carry = body(b * u + j, carry)
            return carry

        return lax.fori_loop(0, NZ // u, step, init)

    for ld in load_rows:
        ld.wait()
    srow_q[...] = srow_q[...] - HR * row_p[...]

    pl.semaphore_wait(barrier, len(peers))
    halo = [
        send(srow_p, rrow_p, hs_sem.at[0], hr_sem.at[0], north),
        send(srow_q, rrow_q, hs_sem.at[1], hr_sem.at[1], south),
    ]

    tell(tok_sem.at[0])

    for a in range(2):
        load_p[a].wait()
        load_e[a].wait()

        def pack(k, z, a=a):
            p = p_v[a, k, own, :]
            edge = jnp.where(lane == CX - 1, p, ew_v[a, k] - HR * p)
            return jnp.where((lane >> 1) == k, pltpu.roll(edge, 2 * k + 1, 1), z)

        z_send[a] = blocked(pack, zero, NZ)
        halo.append(send(z_send.at[a], z_w.at[a], hs_sem.at[2 + a], hr_sem.at[2 + a], east))
        halo.append(send(z_send.at[a], z_e.at[a], hs_sem.at[4 + a], hr_sem.at[4 + a], west))

    load_s.wait()
    load_t.wait()

    def factor(k, carry):
        b_below, rp_below, ts_below, lv = carry
        ss = ss_v[k]
        b = (VR * VR) * ss
        pivot = (1.0 + b + b_below) - b_below * (b_below * rp_below)
        rp = jnp.where(k > 0, 1.0, 0.0) / pivot
        g = b_below * rp
        ts = thick[k] * ss
        lv = (VR * (ts - ts_below)) * rp + g * lv
        rp_v[k] = rp
        g_v[k] = g
        f_v[k] = b * rp
        lam_v[k] = lv
        return b, rp, ts, lv

    blocked(factor, (zero, zero, zero, zero))

    def adjoint(i, carry):
        lam_up, z = carry
        k = NZ - 1 - i
        lam = lam_v[k] + f_v[k] * lam_up
        gg = thick[k] + VR * (lam_up - lam)
        h = gg * ss_v[k]
        lam_v[k] = lam
        c_v[k] = gg - (1.4 * HR) * h
        h_v[k, own, :] = h
        shrow_n[pl.ds(k, 1), :] = h[CY - 1 : CY]
        shrow_s[pl.ds(k, 1), :] = h[0:1]
        hw_v[k] = pltpu.roll(h, 1, 1)
        he_v[k] = pltpu.roll(h, CX - 1, 1)
        return lam, jnp.where((lane >> 1) == k, pltpu.roll(h, 2 * k + 1, 1), z)

    zh_send[...] = blocked(adjoint, (zero, zero))[1]
    pl.semaphore_wait(tok_sem.at[0], len(around))
    halo += [
        send(shrow_n, rhrow_s, hs_sem.at[6], hr_sem.at[6], north),
        send(shrow_s, rhrow_n, hs_sem.at[7], hr_sem.at[7], south),
        send(zh_send, zh_w, hs_sem.at[8], hr_sem.at[8], east),
        send(zh_send, zh_e, hs_sem.at[9], hr_sem.at[9], west),
    ]
    load_n.wait()

    def clear(k, carry):
        for a in range(2):
            p_v[a, k, pl.ds(PAD - 1, 1), :] = line
            p_v[a, k, pl.ds(PAD + CY, 1), :] = line
            nw_v[a, k, pl.ds(PAD + CY, 1), :] = line
        h_v[k, pl.ds(PAD - 1, 1), :] = line
        h_v[k, pl.ds(PAD + CY, 1), :] = line
        return carry

    blocked(clear, 0)
    small = jnp.zeros((8, CX), jnp.float32)

    def inner(b):
        rows = pl.ds(8 * b, 8)
        here, below, above = (pl.ds(PAD + 8 * b + o, 8) for o in (0, -1, 1))

        def body(k, carry):
            hs = HR * ss_v[k, rows, :]
            h = h_v[k, here, :]
            h_below = h_v[k, below, :]
            hw = hw_v[k, rows, :]
            t = thick[k]
            out = []
            for a in range(2):
                s = carry[a]
                p = p_v[a, k, here, :]
                hp = HR * p
                q = ew_v[a, k, rows, :] - hp
                ew1 = q + pltpu.roll(hp, 1, 1)
                nw1 = (nw_v[a, k, here, :] - hp) + HR * p_v[a, k, below, :]
                ee = hp + pltpu.roll(q, CX - 1, 1)
                nn = (nw_v[a, k, above, :] - HR * p_v[a, k, above, :]) + hp
                part_v[a, k, rows, :] = p - hs * ((ee - ew1) + (nn - nw1))
                out.append((
                    s[0] + t * ew1,
                    s[1] + t * nw1,
                    s[2] + h * (ew1 + nw1),
                    s[3] + hw * ew1,
                    s[4] + h_below * nw1,
                ))
            return tuple(out)

        done = blocked(body, ((small,) * 5,) * 2)
        for a in range(2):
            for j in range(5):
                sum_v[j, a, rows, :] = done[a][j]

    for b in range(CY // 8):
        inner(b)

    w_v[:, pl.ds(0, 1), :, :] = jnp.zeros((2, 1, CY, CX), jnp.float32)
    even = (lane & 1) == 0
    odd = (lane & 1) == 1

    def spread(k, t):
        return jnp.where((lane8 >> 1) == k, thick[k], t)

    t_lane = blocked(spread, small, NZ)
    h_first = pltpu.roll(zh_send[...], CX - 1, 1)

    load_w.wait()
    for copy in halo[2:6]:
        copy.wait_recv()

    first_lane = lane == 0
    for a in range(2):
        own_z = z_send[a]
        from_w = jnp.where(even, z_w[a] - own_z, 0.0)
        edge_h[a] = jnp.where(even, from_w, pltpu.roll(z_e[a] - own_z, CX - 2, 1))
        z_w[a] = jnp.where(odd, own_z + HR * pltpu.roll(z_w[a], 1, 1), 0.0)
        t_all = jnp.concatenate([t_lane] * (CY // 8), axis=0)
        more_e = HR * jnp.sum(from_w * t_all, axis=1, keepdims=True)
        more_h = HR * jnp.sum(from_w * h_first, axis=1, keepdims=True)
        sum_v[0, a] += jnp.where(first_lane, more_e, 0.0)
        sum_v[2, a] += jnp.where(first_lane, more_h, 0.0)
    div_lane = jnp.where(lane8 == CX - 1, 1.0, jnp.where(lane8 == 0, -HR, 0.0))

    def forward(blocks):
        def body(k, carry):
            out = []
            for i, b in enumerate(blocks):
                rows = pl.ds(8 * b, 8)
                hs = HR * ss_v[k, rows, :]
                rp = rp_v[k, rows, :]
                g = g_v[k, rows, :]
                for a in range(2):
                    part_below, v = carry[2 * i + a]
                    more = pltpu.roll(edge_h[a, rows, :], 2 * CX - 2 * k, 1) * div_lane
                    if b == 0:
                        more = more - jnp.where(row8 == 0, HR * rrow_p[a, pl.ds(k, 1), :], 0.0)
                    if b == CY // 8 - 1:
                        more = more + jnp.where(row8 == 7, rrow_q[a, pl.ds(k, 1), :], 0.0)
                    part = part_v[a, k, rows, :] - hs * more
                    v = (w_v[a, k, rows, :] - VR * (part - part_below)) * rp + g * v
                    part_v[a, k, rows, :] = part
                    v_v[a, k, rows, :] = v
                    out.append((part, v))
            return tuple(out)

        blocked(body, ((small, small),) * (2 * len(blocks)))

    forward(tuple(range(1, CY // 8 - 1)))
    halo[0].wait_recv()
    halo[1].wait_recv()
    t_rows = jnp.concatenate([jnp.full((1, CX), 0.0, jnp.float32) + thick[k] for k in range(NZ)], axis=0)
    for a in range(2):
        below = HR * rrow_p[a]
        sum_v[1, a, pl.ds(0, 1), :] += jnp.sum(below * t_rows, axis=0, keepdims=True)
        sum_v[2, a, pl.ds(0, 1), :] += jnp.sum(below * shrow_s[...], axis=0, keepdims=True)
        rrow_n[a] = srow_q[a] + below
    forward((0, CY // 8 - 1))

    def backward(b):
        rows = pl.ds(8 * b, 8)
        first, last = b == 0, b == CY // 8 - 1
        pair8 = lane8 >> 1

        def body(i, carry):
            k = NZ - 1 - i
            f = f_v[k, rows, :]
            lam = lam_v[k, rows, :]
            cc0 = c_v[k, rows, :]
            vs = VR * ss_v[k, rows, :]
            hs = h_v[k, pl.ds(PAD - 1 + 8 * b, 8), :]
            hn = h_v[k, pl.ds(PAD + 1 + 8 * b, 8), :]
            hwk = hw_v[k, rows, :]
            hek = he_v[k, rows, :]
            t = thick[k]
            out = []
            for a in range(2):
                w_up, s = carry[a]
                w = v_v[a, k, rows, :] + f * w_up
                p1 = part_v[a, k, rows, :] - vs * (w_up - w)
                if first:
                    edge_n[a, pl.ds(k, 1), :] = p1[0:1]
                if last:
                    edge_p[a, pl.ds(k, 1), :] = p1[7:8]
                s = (
                    s[0] + (cc0 * p1 + lam * w),
                    s[1] + hwk * p1,
                    s[2] + hek * p1,
                    s[3] + hs * p1,
                    s[4] + hn * p1,
                    s[5] + t * p1,
                    jnp.where(pair8 == k, pltpu.roll(p1, 2 * k + 1, 1), s[6]),
                )
                out.append((w, s))
            return tuple(out)

        done = blocked(body, ((small, (small,) * 7),) * 2)
        for a in range(2):
            s = done[a][1]
            acc_v[0, a, rows, :] = s[0] + HR * sum_v[2, a, rows, :]
            acc_v[1, a, rows, :] = (HR * HR) * s[1] - HR * sum_v[3, a, rows, :]
            acc_v[2, a, rows, :] = (HR * HR) * s[2]
            acc_v[3, a, rows, :] = (HR * HR) * s[3] - HR * sum_v[4, a, rows, :]
            acc_v[4, a, rows, :] = (HR * HR) * s[4]
            acc_v[5, a, rows, :] = HR * s[5]
            z_e[a, rows, :] = s[6]

    backward(CY // 8 - 1)
    backward(0)

    rn_send[...] = jnp.zeros_like(rn_send)
    rs_send[...] = jnp.zeros_like(rs_send)
    halo[6].wait_recv()
    halo[7].wait_recv()
    tell(tok_sem.at[1])
    for a in range(2):
        rn_send[a : a + 1, :] = (HR * HR) * jnp.sum(rhrow_n[...] * edge_p[a], axis=0, keepdims=True)
        rn_send[2 + a : 3 + a, :] = acc_v[5, a, pl.ds(CY - 1, 1), :]
        rs_send[a : a + 1, :] = HR * jnp.sum(
            rhrow_s[...] * (HR * edge_n[a] - rrow_n[a]), axis=0, keepdims=True
        )
    send(rn_send, rs_recv.at[m], rns_sem.at[0], rsr_sem.at[m], (0, rr(1), c))
    send(rs_send, rn_recv.at[m], rss_sem.at[0], rnr_sem.at[m], (NM - 1, rr(-1), c))

    for b in range(1, CY // 8 - 1):
        backward(b)

    halo[8].wait_recv()
    halo[9].wait_recv()

    to_e, to_w = zero, zero
    h_west = pltpu.roll(zh_w[...], 1, 1)
    h_east = pltpu.roll(zh_e[...], CX - 1, 1)
    for a in range(2):
        base, xe, xw, xn, xs, hp = (acc_v[j, a] for j in range(6))
        mass = (
            base
            + jnp.where(lane == CX - 1, 0.0, pltpu.roll(xe, CX - 1, 1))
            + jnp.where(lane == 0, 0.0, pltpu.roll(xw, 1, 1))
            + jnp.where(row == CY - 1, 0.0, pltpu.roll(xn, CY - 1, 0))
            + jnp.where(row == 0, 0.0, pltpu.roll(xs, 1, 0))
        )
        e2 = sum_v[0, a] - (hp - jnp.where(lane == 0, 0.0, pltpu.roll(hp, 1, 1)))
        n2 = sum_v[1, a] - (hp - jnp.where(row == 0, 0.0, pltpu.roll(hp, 1, 0)))
        for q in range(NM):
            i_send[q, 3 * a] = mass[q * Q : (q + 1) * Q]
            i_send[q, 3 * a + 1] = e2[q * Q : (q + 1) * Q]
            i_send[q, 3 * a + 2] = n2[q * Q : (q + 1) * Q]
        ends = z_e[a]
        xw_last = (HR * HR) * jnp.sum(jnp.where(even, h_east * ends, 0.0), axis=1, keepdims=True)
        xe_first = HR * jnp.sum(jnp.where(odd, h_west * (HR * ends - z_w[a]), 0.0), axis=1, keepdims=True)
        to_e = jnp.where(lane == a, xw_last, to_e)
        to_e = jnp.where(lane == 2 + a, pltpu.roll(hp, a + 3, 1), to_e)
        to_w = jnp.where(lane == a, xe_first, to_w)
    for q in range(NM):
        ce_send[q] = to_e[q * Q : (q + 1) * Q]
        cw_send[q] = to_w[q * Q : (q + 1) * Q]

    for d in range(NM):
        q = mm(d)
        send(ce_send.at[q], ce_recv.at[m], ces_sem.at[q], cer_sem.at[m], (q, r, cc(1)))
        send(cw_send.at[q], cw_recv.at[m], cws_sem.at[q], cwr_sem.at[m], (q, r, cc(-1)))
    for d in range(1, NM):
        q = mm(d)
        send(i_send.at[q], i_recv.at[m], is_sem.at[q], ir_sem.at[m], (q, r, c))
    i_recv[m] = i_send[m]

    for d in range(1, NM):
        arrived(i_recv, ir_sem, mm(d))
    for d in range(NM):
        arrived(ce_recv, cer_sem, mm(d))
        arrived(cw_recv, cwr_sem, mm(d))

    @pl.when(m == 0)
    def _():
        for d in range(NM):
            arrived(rs_recv, rsr_sem, mm(d))
        for s in range(NM):
            for a in range(2):
                i_recv[s, 3 * a, 0:1, :] += rs_recv[s, a : a + 1, :]
                i_recv[s, 3 * a + 2, 0:1, :] += rs_recv[s, 2 + a : 3 + a, :]

    @pl.when(m == NM - 1)
    def _():
        for d in range(NM):
            arrived(rn_recv, rnr_sem, mm(d))
        for s in range(NM):
            for a in range(2):
                i_recv[s, 3 * a, Q - 1 : Q, :] += rn_recv[s, a : a + 1, :]

    members = 2 * NM
    fields = ([], [], [])
    for s in range(NM):
        ce = ce_recv[s]
        cw = cw_recv[s]
        for a in range(2):
            mass = i_recv[s, 3 * a]
            mass += jnp.where(lane8 == 0, pltpu.roll(ce, CX - a, 1) if a else ce, 0.0)
            mass += jnp.where(lane8 == CX - 1, pltpu.roll(cw, CX - 1 - a, 1), 0.0)
            e2 = i_recv[s, 3 * a + 1]
            e2 += jnp.where(lane8 == 0, pltpu.roll(ce, CX - 2 - a, 1), 0.0)
            fields[0].append(mass)
            fields[1].append(e2)
            fields[2].append(i_recv[s, 3 * a + 2])
    for j in range(3):
        mean = sum(fields[j][1:], fields[j][0]) * (1.0 / members)
        devs = [(x - mean) * (x - mean) for x in fields[j]]
        gath_a[c, j] = mean
        gath_b[r, j] = sum(devs[1:], devs[0]) * (1.0 / (members - 1))

    def far(n):
        return sorted(range(1, n), key=lambda d: -min(d, n - d))

    pl.semaphore_wait(tok_sem.at[1], len(around))
    for d in far(NC):
        send(gath_a.at[c], gath_a.at[c], ga_s.at[d], ga_r.at[c], (m, r, cc(d)))
    for d in far(NR):
        send(gath_b.at[r], gath_b.at[r], gb_s.at[d], gb_r.at[r], (m, rr(d), c))

    load_o.wait()
    wanted = [rr(d) * NC + c for d in range(NR)] + [r * NC + cc(d) for d in range(1, NC)]

    def find(i, got):
        for j in range(8 if NR * NC % 8 == 0 else 1):
            t = i * (8 if NR * NC % 8 == 0 else 1) + j
            o = owner[t]
            got = tuple(jnp.where(o == w, t, g) for w, g in zip(wanted, got))
        return got

    steps = NR * NC // 8 if NR * NC % 8 == 0 else NR * NC
    source = lax.fori_loop(0, steps, find, tuple(jnp.int32(0) for _ in wanted))
    col_source, row_source = source[:NR], source[:1] + source[NR:]

    for d in range(1, NC):
        arrived(gath_a, ga_r, cc(d))
    for d in far(NR):
        send_a[d] = gath_a[lax.rem(col_source[d], NC)]
        send(send_a.at[d], recv_a.at[r], sa_s.at[d], sa_r.at[r], (m, rr(d), c))
    for d in range(1, NR):
        arrived(gath_b, gb_r, rr(d))
    for d in far(NC):
        send_b[d] = gath_b[row_source[d] // NC]
        send(send_b.at[d], recv_b.at[c], sb_s.at[d], sb_r.at[c], (m, r, cc(d)))
    recv_a[r] = gath_a[lax.rem(source[0], NC)]
    recv_b[c] = gath_b[source[0] // NC]
    for d in range(1, NR):
        arrived(recv_a, sa_r, rr(d))
    for d in range(1, NC):
        arrived(recv_b, sb_r, cc(d))
    out_ref[0, 0, 0:3] = recv_a[source[0] // NC]
    out_ref[0, 0, 3:6] = recv_b[lax.rem(source[0], NC)]
    for copy in sends:
        copy.wait_send()


def local(dims, pressure, east_wind, north_wind, vertical_wind, sound_squared, thickness, owner_map):
    NM, NR, NC, NZ, CY, CX, U = dims
    Q = CY // NM
    f32 = jnp.float32
    V = pltpu.VMEM
    D = pltpu.SemaphoreType.DMA
    rows = CY + 2 * PAD
    two = (2, NZ, CY, CX)
    one = (NZ, CY, CX)
    tile = (CY, CX)
    pair = (2, CY, CX)
    scratch = [
        pltpu.SMEM((NZ,), f32), pltpu.SMEM((NR * NC,), jnp.int32),
        V((2, NZ, rows, CX), f32), V(two, f32), V((2, NZ, rows, CX), f32), V(two, f32), V(one, f32),
        V(two, f32), V(two, f32),
        V(one, f32), V(one, f32), V(one, f32), V(one, f32), V(one, f32),
        V((NZ, rows, CX), f32), V(one, f32), V(one, f32),
        V(pair, f32), V((2, NZ, CX), f32), V((2, NZ, CX), f32), V((2, NZ, CX), f32),
        V(tile, f32), V((NZ, CX), f32), V((NZ, CX), f32),
        V((2, NZ, CX), f32), V((2, NZ, CX), f32), V((2, NZ, CX), f32),
        V(pair, f32), V(pair, f32), V((2, NZ, CX), f32), V((2, NZ, CX), f32),
        V(tile, f32), V(tile, f32), V((NZ, CX), f32), V((NZ, CX), f32),
        V(pair, f32), V((5, 2, CY, CX), f32), V((6, 2, CY, CX), f32), V((NM, 6, Q, CX), f32), V((NM, 6, Q, CX), f32),
        V((NM, Q, CX), f32), V((NM, Q, CX), f32), V((NM, Q, CX), f32), V((NM, Q, CX), f32),
        V((8, CX), f32), V((8, CX), f32), V((NM, 8, CX), f32), V((NM, 8, CX), f32),
        V((NC, 3, Q, CX), f32), V((NR, 3, Q, CX), f32),
        V((NR, 3, Q, CX), f32), V((NC, 3, Q, CX), f32),
        V((NR, 3, Q, CX), f32), V((NC, 3, Q, CX), f32),
        pltpu.SemaphoreType.REGULAR((2,)), D((12,)), D((10,)), D((10,)), D((NM,)), D((NM,)),
        D((NM,)), D((NM,)), D((NM,)), D((NM,)),
        D((1,)), D((NM,)), D((1,)), D((NM,)),
        D((NC,)), D((NC,)), D((NR,)), D((NR,)), D((NR,)), D((NR,)), D((NC,)), D((NC,)),
    ]
    hbm = pl.BlockSpec(memory_space=pl.ANY)
    small = [pltpu.with_memory_space_constraint(x, pltpu.HBM) for x in (thickness, owner_map)]
    return pl.pallas_call(
        functools.partial(kernel, dims),
        out_shape=jax.ShapeDtypeStruct((1, 1, 6, Q, CX), f32),
        in_specs=[hbm] * 7,
        out_specs=pl.BlockSpec(memory_space=pltpu.VMEM),
        scratch_shapes=scratch,
        compiler_params=pltpu.CompilerParams(
            collective_id=0, has_side_effects=True, vmem_limit_bytes=54500 * 1024
        ),
        name="substeps",
    )(*small, pressure, east_wind, north_wind, vertical_wind, sound_squared)


def solution(mesh):
    placed = (
        P("mem", None, "ty", "tx"),
        P("mem", None, "ty", "tx"),
        P("mem", None, "ty", "tx"),
        P("mem", None, "ty", "tx"),
        P(None, "ty", "tx"),
        P(),
        P(),
    )

    def step(*args):
        levels = args[0].shape[1]
        dims = (
            mesh.shape["mem"], mesh.shape["ty"], mesh.shape["tx"], levels,
            args[0].shape[2] , args[0].shape[3], 25 if levels % 25 == 0 else 1,
        )
        return local(dims, *args)

    return jax.shard_map(
        step,
        mesh=mesh,
        in_specs=placed,
        out_specs=P("ty", "tx", None, "mem", None),
        check_vma=False,
    )
```

```python
import functools

import jax
import jax.numpy as jnp
from jax import lax
from jax.experimental import pallas as pl
from jax.experimental.pallas import tpu as pltpu
from jax.sharding import PartitionSpec as P

HR = 0.35
VR = 1.5
PAD = 8
MESH = pl.DeviceIdType.MESH


def kernel(dims, thick_h, owner_h, p_h, ew_h, nw_h, w_h, ss_h, out_ref, *scratch):
    NM, NR, NC, NZ, CY, CX, U = dims
    (
        thick, owner,
        p_v, ew_v, nw_v, w_v, ss_v, part_v, v_v,
        rp_v, g_v, f_v, lam_v, c_v, h_v, hw_v, he_v,
        z_send, srow_p, srow_q, row_p, zh_send, shrow_n, shrow_s, edge_p, edge_n, rrow_n,
        z_w, z_e, rrow_p, rrow_q, zh_w, zh_e, rhrow_s, rhrow_n,
        edge_h, sum_v, acc_v, i_send, i_recv, ce_send, cw_send, ce_recv, cw_recv,
        rn_send, rs_send, rs_recv, rn_recv,
        gath_a, gath_b, send_a, send_b, recv_a, recv_b,
        tok_sem, ld_sem, hs_sem, hr_sem, is_sem, ir_sem, ces_sem, cer_sem, cws_sem, cwr_sem,
        rns_sem, rsr_sem, rss_sem, rnr_sem,
        ga_s, ga_r, gb_s, gb_r, sa_s, sa_r, sb_s, sb_r,
    ) = scratch
    Q = CY // NM
    m = lax.axis_index("mem")
    r = lax.axis_index("ty")
    c = lax.axis_index("tx")

    def mm(d):
        return lax.rem(m + d, NM)

    def rr(d):
        return lax.rem(r + d + NR, NR)

    def cc(d):
        return lax.rem(c + d + NC, NC)

    own = pl.ds(PAD, CY)
    load_p = [pltpu.make_async_copy(p_h.at[a], p_v.at[a, :, own, :], ld_sem.at[a]) for a in range(2)]
    load_e = [pltpu.make_async_copy(ew_h.at[a], ew_v.at[a], ld_sem.at[2 + a]) for a in range(2)]
    load_n = pltpu.make_async_copy(nw_h, nw_v.at[:, :, own, :], ld_sem.at[4])
    load_s = pltpu.make_async_copy(ss_h, ss_v, ld_sem.at[5])
    load_w = pltpu.make_async_copy(w_h, w_v.at[:, pl.ds(1, NZ - 1), :, :], ld_sem.at[6])
    load_t = pltpu.make_async_copy(thick_h, thick, ld_sem.at[7])
    load_o = pltpu.make_async_copy(owner_h, owner, ld_sem.at[8])
    load_rows = [
        pltpu.make_async_copy(p_h.at[:, :, CY - 1, :], srow_p, ld_sem.at[9]),
        pltpu.make_async_copy(p_h.at[:, :, 0, :], row_p, ld_sem.at[10]),
        pltpu.make_async_copy(nw_h.at[:, :, 0, :], srow_q, ld_sem.at[11]),
    ]
    for ld in (load_s, load_t, load_p[0], load_e[0], *load_rows, load_p[1], load_e[1], load_n, load_w, load_o):
        ld.start()

    barrier = pltpu.get_barrier_semaphore()
    east, west = (m, r, cc(1)), (m, r, cc(-1))
    north, south = (m, rr(1), c), (m, rr(-1), c)
    around = (north, south, east, west)
    peers = [*around, *((mm(d), r, c) for d in range(1, NM))]
    for peer in peers:
        pl.semaphore_signal(barrier, inc=1, device_id=peer, device_id_type=MESH)

    sends = []

    def send(src, dst, ssem, rsem, dev):
        copy = pltpu.make_async_remote_copy(
            src_ref=src, dst_ref=dst, send_sem=ssem, recv_sem=rsem,
            device_id=dev, device_id_type=MESH,
        )
        copy.start()
        sends.append(copy)
        return copy

    def arrived(ref, sem, slot):
        pltpu.make_async_copy(ref.at[slot], ref.at[slot], sem.at[slot]).wait()

    def tell(sem):
        for peer in around:
            pl.semaphore_signal(sem, inc=1, device_id=peer, device_id_type=MESH)

    lane = lax.broadcasted_iota(jnp.int32, (CY, CX), 1)
    row = lax.broadcasted_iota(jnp.int32, (CY, CX), 0)
    lane8 = lax.broadcasted_iota(jnp.int32, (8, CX), 1)
    row8 = lax.broadcasted_iota(jnp.int32, (8, CX), 0)
    zero = jnp.zeros((CY, CX), jnp.float32)
    line = jnp.zeros((1, CX), jnp.float32)

    def blocked(body, init, u=U):
        if u >= NZ:
            for k in range(NZ):
                init = body(k, init)
            return init

        def step(b, carry):
            for j in range(u):
                carry = body(b * u + j, carry)
            return carry

        return lax.fori_loop(0, NZ // u, step, init)

    def pack(a):
        load_p[a].wait()
        load_e[a].wait()

        def body(k, z):
            p = p_v[a, k, own, :]
            edge = jnp.where(lane == CX - 1, p, ew_v[a, k] - HR * p)
            return jnp.where((lane >> 1) == k, pltpu.roll(edge, 2 * k + 1, 1), z)

        z_send[a] = blocked(body, zero, NZ)

    def send_edges(a):
        return [
            send(z_send.at[a], z_w.at[a], hs_sem.at[2 + a], hr_sem.at[2 + a], east),
            send(z_send.at[a], z_e.at[a], hs_sem.at[4 + a], hr_sem.at[4 + a], west),
        ]

    load_s.wait()
    load_t.wait()

    def factor(k, carry):
        b_below, rp_below, ts_below, lv = carry
        ss = ss_v[k]
        b = (VR * VR) * ss
        pivot = (1.0 + b + b_below) - b_below * (b_below * rp_below)
        rp = jnp.where(k > 0, 1.0, 0.0) / pivot
        g = b_below * rp
        ts = thick[k] * ss
        lv = (VR * (ts - ts_below)) * rp + g * lv
        rp_v[k] = rp
        g_v[k] = g
        f_v[k] = b * rp
        lam_v[k] = lv
        return b, rp, ts, lv

    blocked(factor, (zero, zero, zero, zero), NZ)

    pack(0)
    for ld in load_rows:
        ld.wait()
    srow_q[...] = srow_q[...] - HR * row_p[...]

    pl.semaphore_wait(barrier, len(peers))
    halo = [
        send(srow_p, rrow_p, hs_sem.at[0], hr_sem.at[0], north),
        send(srow_q, rrow_q, hs_sem.at[1], hr_sem.at[1], south),
    ]
    tell(tok_sem.at[0])
    halo += send_edges(0)
    pack(1)
    halo += send_edges(1)

    def adjoint(i, carry):
        lam_up, z = carry
        k = NZ - 1 - i
        lam = lam_v[k] + f_v[k] * lam_up
        gg = thick[k] + VR * (lam_up - lam)
        h = gg * ss_v[k]
        lam_v[k] = lam
        c_v[k] = gg - (1.4 * HR) * h
        h_v[k, own, :] = h
        shrow_n[pl.ds(k, 1), :] = h[CY - 1 : CY]
        shrow_s[pl.ds(k, 1), :] = h[0:1]
        return lam, jnp.where((lane >> 1) == k, pltpu.roll(h, 2 * k + 1, 1), z)

    zh_send[...] = blocked(adjoint, (zero, zero), NZ)[1]
    halo += [
        send(shrow_n, rhrow_s, hs_sem.at[6], hr_sem.at[6], north),
        send(shrow_s, rhrow_n, hs_sem.at[7], hr_sem.at[7], south),
        send(zh_send, zh_w, hs_sem.at[8], hr_sem.at[8], east),
        send(zh_send, zh_e, hs_sem.at[9], hr_sem.at[9], west),
    ]
    load_n.wait()

    def clear(k, carry):
        for a in range(2):
            p_v[a, k, pl.ds(PAD - 1, 1), :] = line
            p_v[a, k, pl.ds(PAD + CY, 1), :] = line
            nw_v[a, k, pl.ds(PAD + CY, 1), :] = line
        h_v[k, pl.ds(PAD - 1, 1), :] = line
        h_v[k, pl.ds(PAD + CY, 1), :] = line
        return carry

    blocked(clear, 0)
    small = jnp.zeros((8, CX), jnp.float32)

    def inner(b):
        rows = pl.ds(8 * b, 8)
        here, below, above = (pl.ds(PAD + 8 * b + o, 8) for o in (0, -1, 1))

        def body(k, carry):
            hs = HR * ss_v[k, rows, :]
            h = h_v[k, here, :]
            h_below = h_v[k, below, :]
            hw = pltpu.roll(h, 1, 1)
            hw_v[k, rows, :] = hw
            he_v[k, rows, :] = pltpu.roll(h, CX - 1, 1)
            t = thick[k]
            out = []
            for a in range(2):
                s = carry[a]
                p = p_v[a, k, here, :]
                hp = HR * p
                q = ew_v[a, k, rows, :] - hp
                ew1 = q + pltpu.roll(hp, 1, 1)
                nw1 = (nw_v[a, k, here, :] - hp) + HR * p_v[a, k, below, :]
                ee = hp + pltpu.roll(q, CX - 1, 1)
                nn = (nw_v[a, k, above, :] - HR * p_v[a, k, above, :]) + hp
                part_v[a, k, rows, :] = p - hs * ((ee - ew1) + (nn - nw1))
                out.append((
                    s[0] + t * ew1,
                    s[1] + t * nw1,
                    s[2] + h * (ew1 + nw1),
                    s[3] + hw * ew1,
                    s[4] + h_below * nw1,
                ))
            return tuple(out)

        done = blocked(body, ((small,) * 5,) * 2, NZ)
        for a in range(2):
            for j in range(5):
                sum_v[j, a, rows, :] = done[a][j]

    inner(0)
    inner(1)
    pl.semaphore_wait(tok_sem.at[0], len(around))
    tell(tok_sem.at[1])
    for b in range(2, CY // 8):
        inner(b)

    w_v[:, pl.ds(0, 1), :, :] = jnp.zeros((2, 1, CY, CX), jnp.float32)
    even = (lane & 1) == 0
    odd = (lane & 1) == 1

    def spread(k, t):
        return jnp.where((lane8 >> 1) == k, thick[k], t)

    t_lane = blocked(spread, small, NZ)
    h_first = pltpu.roll(zh_send[...], CX - 1, 1)

    load_w.wait()
    for copy in halo[2:6]:
        copy.wait_recv()

    first_lane = lane == 0
    for a in range(2):
        own_z = z_send[a]
        from_w = jnp.where(even, z_w[a] - own_z, 0.0)
        edge_h[a] = jnp.where(even, from_w, pltpu.roll(z_e[a] - own_z, CX - 2, 1))
        z_w[a] = jnp.where(odd, own_z + HR * pltpu.roll(z_w[a], 1, 1), 0.0)
        t_all = jnp.concatenate([t_lane] * (CY // 8), axis=0)
        more_e = HR * jnp.sum(from_w * t_all, axis=1, keepdims=True)
        more_h = HR * jnp.sum(from_w * h_first, axis=1, keepdims=True)
        sum_v[0, a] += jnp.where(first_lane, more_e, 0.0)
        sum_v[2, a] += jnp.where(first_lane, more_h, 0.0)
    div_lane = jnp.where(lane8 == CX - 1, 1.0, jnp.where(lane8 == 0, -HR, 0.0))

    def forward(blocks):
        def body(k, carry):
            out = []
            for i, b in enumerate(blocks):
                rows = pl.ds(8 * b, 8)
                hs = HR * ss_v[k, rows, :]
                rp = rp_v[k, rows, :]
                g = g_v[k, rows, :]
                for a in range(2):
                    part_below, v = carry[2 * i + a]
                    more = pltpu.roll(edge_h[a, rows, :], 2 * CX - 2 * k, 1) * div_lane
                    if b == 0:
                        more = more - jnp.where(row8 == 0, HR * rrow_p[a, pl.ds(k, 1), :], 0.0)
                    if b == CY // 8 - 1:
                        more = more + jnp.where(row8 == 7, rrow_q[a, pl.ds(k, 1), :], 0.0)
                    part = part_v[a, k, rows, :] - hs * more
                    v = (w_v[a, k, rows, :] - VR * (part - part_below)) * rp + g * v
                    part_v[a, k, rows, :] = part
                    v_v[a, k, rows, :] = v
                    out.append((part, v))
            return tuple(out)

        blocked(body, ((small, small),) * (2 * len(blocks)), NZ)

    forward(tuple(range(1, CY // 8 - 1)))
    halo[0].wait_recv()
    halo[1].wait_recv()
    t_rows = jnp.concatenate([jnp.full((1, CX), 0.0, jnp.float32) + thick[k] for k in range(NZ)], axis=0)
    for a in range(2):
        below = HR * rrow_p[a]
        sum_v[1, a, pl.ds(0, 1), :] += jnp.sum(below * t_rows, axis=0, keepdims=True)
        sum_v[2, a, pl.ds(0, 1), :] += jnp.sum(below * shrow_s[...], axis=0, keepdims=True)
        rrow_n[a] = srow_q[a] + below
    forward((0, CY // 8 - 1))

    def backward(blocks):
        pair8 = lane8 >> 1

        def body(i, carry):
            k = NZ - 1 - i
            t = thick[k]
            out = []
            for n, b in enumerate(blocks):
                rows = pl.ds(8 * b, 8)
                f = f_v[k, rows, :]
                lam = lam_v[k, rows, :]
                cc0 = c_v[k, rows, :]
                vs = VR * ss_v[k, rows, :]
                hs = h_v[k, pl.ds(PAD - 1 + 8 * b, 8), :]
                hn = h_v[k, pl.ds(PAD + 1 + 8 * b, 8), :]
                hwk = hw_v[k, rows, :]
                hek = he_v[k, rows, :]
                for a in range(2):
                    w_up, s = carry[2 * n + a]
                    w = v_v[a, k, rows, :] + f * w_up
                    p1 = part_v[a, k, rows, :] - vs * (w_up - w)
                    if b == 0:
                        edge_n[a, pl.ds(k, 1), :] = p1[0:1]
                    if b == CY // 8 - 1:
                        edge_p[a, pl.ds(k, 1), :] = p1[7:8]
                    s = (
                        s[0] + (cc0 * p1 + lam * w),
                        s[1] + hwk * p1,
                        s[2] + hek * p1,
                        s[3] + hs * p1,
                        s[4] + hn * p1,
                        s[5] + t * p1,
                        jnp.where(pair8 == k, pltpu.roll(p1, 2 * k + 1, 1), s[6]),
                    )
                    out.append((w, s))
            return tuple(out)

        done = blocked(body, ((small, (small,) * 7),) * (2 * len(blocks)), NZ)
        for n, b in enumerate(blocks):
            rows = pl.ds(8 * b, 8)
            for a in range(2):
                s = done[2 * n + a][1]
                acc_v[0, a, rows, :] = s[0] + HR * sum_v[2, a, rows, :]
                acc_v[1, a, rows, :] = (HR * HR) * s[1] - HR * sum_v[3, a, rows, :]
                acc_v[2, a, rows, :] = (HR * HR) * s[2]
                acc_v[3, a, rows, :] = (HR * HR) * s[3] - HR * sum_v[4, a, rows, :]
                acc_v[4, a, rows, :] = (HR * HR) * s[4]
                acc_v[5, a, rows, :] = HR * s[5]
                z_e[a, rows, :] = s[6]

    backward((0, CY // 8 - 1))

    rn_send[...] = jnp.zeros_like(rn_send)
    rs_send[...] = jnp.zeros_like(rs_send)
    halo[6].wait_recv()
    halo[7].wait_recv()
    pl.semaphore_wait(tok_sem.at[1], len(around))
    tell(tok_sem.at[2])
    for a in range(2):
        rn_send[a : a + 1, :] = (HR * HR) * jnp.sum(rhrow_n[...] * edge_p[a], axis=0, keepdims=True)
        rn_send[2 + a : 3 + a, :] = acc_v[5, a, pl.ds(CY - 1, 1), :]
        rs_send[a : a + 1, :] = HR * jnp.sum(
            rhrow_s[...] * (HR * edge_n[a] - rrow_n[a]), axis=0, keepdims=True
        )
    send(rn_send, rs_recv.at[m], rns_sem.at[0], rsr_sem.at[m], (0, rr(1), c))
    send(rs_send, rn_recv.at[m], rss_sem.at[0], rnr_sem.at[m], (NM - 1, rr(-1), c))

    backward(tuple(range(1, CY // 8 - 1)))

    halo[8].wait_recv()
    halo[9].wait_recv()

    to_e, to_w = zero, zero
    h_west = pltpu.roll(zh_w[...], 1, 1)
    h_east = pltpu.roll(zh_e[...], CX - 1, 1)
    for a in range(2):
        base, xe, xw, xn, xs, hp = (acc_v[j, a] for j in range(6))
        mass = (
            base
            + jnp.where(lane == CX - 1, 0.0, pltpu.roll(xe, CX - 1, 1))
            + jnp.where(lane == 0, 0.0, pltpu.roll(xw, 1, 1))
            + jnp.where(row == CY - 1, 0.0, pltpu.roll(xn, CY - 1, 0))
            + jnp.where(row == 0, 0.0, pltpu.roll(xs, 1, 0))
        )
        e2 = sum_v[0, a] - (hp - jnp.where(lane == 0, 0.0, pltpu.roll(hp, 1, 1)))
        n2 = sum_v[1, a] - (hp - jnp.where(row == 0, 0.0, pltpu.roll(hp, 1, 0)))
        for q in range(NM):
            i_send[q, 3 * a] = mass[q * Q : (q + 1) * Q]
            i_send[q, 3 * a + 1] = e2[q * Q : (q + 1) * Q]
            i_send[q, 3 * a + 2] = n2[q * Q : (q + 1) * Q]
        ends = z_e[a]
        xw_last = (HR * HR) * jnp.sum(jnp.where(even, h_east * ends, 0.0), axis=1, keepdims=True)
        xe_first = HR * jnp.sum(jnp.where(odd, h_west * (HR * ends - z_w[a]), 0.0), axis=1, keepdims=True)
        to_e = jnp.where(lane == a, xw_last, to_e)
        to_e = jnp.where(lane == 2 + a, pltpu.roll(hp, a + 3, 1), to_e)
        to_w = jnp.where(lane == a, xe_first, to_w)
    for q in range(NM):
        ce_send[q] = to_e[q * Q : (q + 1) * Q]
        cw_send[q] = to_w[q * Q : (q + 1) * Q]

    for d in range(NM):
        q = mm(d)
        send(ce_send.at[q], ce_recv.at[m], ces_sem.at[q], cer_sem.at[m], (q, r, cc(1)))
        send(cw_send.at[q], cw_recv.at[m], cws_sem.at[q], cwr_sem.at[m], (q, r, cc(-1)))
    for d in range(1, NM):
        q = mm(d)
        send(i_send.at[q], i_recv.at[m], is_sem.at[q], ir_sem.at[m], (q, r, c))
    i_recv[m] = i_send[m]

    for d in range(1, NM):
        arrived(i_recv, ir_sem, mm(d))
    for d in range(NM):
        arrived(ce_recv, cer_sem, mm(d))
        arrived(cw_recv, cwr_sem, mm(d))

    @pl.when(m == 0)
    def _():
        for d in range(NM):
            arrived(rs_recv, rsr_sem, mm(d))
        for s in range(NM):
            for a in range(2):
                i_recv[s, 3 * a, 0:1, :] += rs_recv[s, a : a + 1, :]
                i_recv[s, 3 * a + 2, 0:1, :] += rs_recv[s, 2 + a : 3 + a, :]

    @pl.when(m == NM - 1)
    def _():
        for d in range(NM):
            arrived(rn_recv, rnr_sem, mm(d))
        for s in range(NM):
            for a in range(2):
                i_recv[s, 3 * a, Q - 1 : Q, :] += rn_recv[s, a : a + 1, :]

    members = 2 * NM
    fields = ([], [], [])
    for s in range(NM):
        ce = ce_recv[s]
        cw = cw_recv[s]
        for a in range(2):
            mass = i_recv[s, 3 * a]
            mass += jnp.where(lane8 == 0, pltpu.roll(ce, CX - a, 1) if a else ce, 0.0)
            mass += jnp.where(lane8 == CX - 1, pltpu.roll(cw, CX - 1 - a, 1), 0.0)
            e2 = i_recv[s, 3 * a + 1]
            e2 += jnp.where(lane8 == 0, pltpu.roll(ce, CX - 2 - a, 1), 0.0)
            fields[0].append(mass)
            fields[1].append(e2)
            fields[2].append(i_recv[s, 3 * a + 2])
    for j in range(3):
        mean = sum(fields[j][1:], fields[j][0]) * (1.0 / members)
        devs = [(x - mean) * (x - mean) for x in fields[j]]
        gath_a[c, j] = mean
        gath_b[r, j] = sum(devs[1:], devs[0]) * (1.0 / (members - 1))

    def far(n):
        return sorted(range(1, n), key=lambda d: -min(d, n - d))

    pl.semaphore_wait(tok_sem.at[2], len(around))
    for d in far(NC):
        send(gath_a.at[c], gath_a.at[c], ga_s.at[d], ga_r.at[c], (m, r, cc(d)))
    for d in far(NR):
        send(gath_b.at[r], gath_b.at[r], gb_s.at[d], gb_r.at[r], (m, rr(d), c))

    load_o.wait()
    wanted = [rr(d) * NC + c for d in range(NR)] + [r * NC + cc(d) for d in range(1, NC)]

    def find(i, got):
        for j in range(8 if NR * NC % 8 == 0 else 1):
            t = i * (8 if NR * NC % 8 == 0 else 1) + j
            o = owner[t]
            got = tuple(jnp.where(o == w, t, g) for w, g in zip(wanted, got))
        return got

    steps = NR * NC // 8 if NR * NC % 8 == 0 else NR * NC
    source = lax.fori_loop(0, steps, find, tuple(jnp.int32(0) for _ in wanted))
    col_source, row_source = source[:NR], source[:1] + source[NR:]

    for d in range(1, NC):
        arrived(gath_a, ga_r, cc(d))
    for d in far(NR):
        send_a[d] = gath_a[lax.rem(col_source[d], NC)]
        send(send_a.at[d], recv_a.at[r], sa_s.at[d], sa_r.at[r], (m, rr(d), c))
    for d in range(1, NR):
        arrived(gath_b, gb_r, rr(d))
    for d in far(NC):
        send_b[d] = gath_b[row_source[d] // NC]
        send(send_b.at[d], recv_b.at[c], sb_s.at[d], sb_r.at[c], (m, r, cc(d)))
    recv_a[r] = gath_a[lax.rem(source[0], NC)]
    recv_b[c] = gath_b[source[0] // NC]
    for d in range(1, NR):
        arrived(recv_a, sa_r, rr(d))
    for d in range(1, NC):
        arrived(recv_b, sb_r, cc(d))
    out_ref[0, 0, 0:3] = recv_a[source[0] // NC]
    out_ref[0, 0, 3:6] = recv_b[lax.rem(source[0], NC)]
    for copy in sends:
        copy.wait_send()


def local(dims, pressure, east_wind, north_wind, vertical_wind, sound_squared, thickness, owner_map):
    NM, NR, NC, NZ, CY, CX, U = dims
    Q = CY // NM
    f32 = jnp.float32
    V = pltpu.VMEM
    D = pltpu.SemaphoreType.DMA
    rows = CY + 2 * PAD
    two = (2, NZ, CY, CX)
    one = (NZ, CY, CX)
    tile = (CY, CX)
    pair = (2, CY, CX)
    scratch = [
        pltpu.SMEM((NZ,), f32), pltpu.SMEM((NR * NC,), jnp.int32),
        V((2, NZ, rows, CX), f32), V(two, f32), V((2, NZ, rows, CX), f32), V(two, f32), V(one, f32),
        V(two, f32), V(two, f32),
        V(one, f32), V(one, f32), V(one, f32), V(one, f32), V(one, f32),
        V((NZ, rows, CX), f32), V(one, f32), V(one, f32),
        V(pair, f32), V((2, NZ, CX), f32), V((2, NZ, CX), f32), V((2, NZ, CX), f32),
        V(tile, f32), V((NZ, CX), f32), V((NZ, CX), f32),
        V((2, NZ, CX), f32), V((2, NZ, CX), f32), V((2, NZ, CX), f32),
        V(pair, f32), V(pair, f32), V((2, NZ, CX), f32), V((2, NZ, CX), f32),
        V(tile, f32), V(tile, f32), V((NZ, CX), f32), V((NZ, CX), f32),
        V(pair, f32), V((5, 2, CY, CX), f32), V((6, 2, CY, CX), f32), V((NM, 6, Q, CX), f32), V((NM, 6, Q, CX), f32),
        V((NM, Q, CX), f32), V((NM, Q, CX), f32), V((NM, Q, CX), f32), V((NM, Q, CX), f32),
        V((8, CX), f32), V((8, CX), f32), V((NM, 8, CX), f32), V((NM, 8, CX), f32),
        V((NC, 3, Q, CX), f32), V((NR, 3, Q, CX), f32),
        V((NR, 3, Q, CX), f32), V((NC, 3, Q, CX), f32),
        V((NR, 3, Q, CX), f32), V((NC, 3, Q, CX), f32),
        pltpu.SemaphoreType.REGULAR((3,)), D((12,)), D((10,)), D((10,)), D((NM,)), D((NM,)),
        D((NM,)), D((NM,)), D((NM,)), D((NM,)),
        D((1,)), D((NM,)), D((1,)), D((NM,)),
        D((NC,)), D((NC,)), D((NR,)), D((NR,)), D((NR,)), D((NR,)), D((NC,)), D((NC,)),
    ]
    hbm = pl.BlockSpec(memory_space=pl.ANY)
    small = [pltpu.with_memory_space_constraint(x, pltpu.HBM) for x in (thickness, owner_map)]
    return pl.pallas_call(
        functools.partial(kernel, dims),
        out_shape=jax.ShapeDtypeStruct((1, 1, 6, Q, CX), f32),
        in_specs=[hbm] * 7,
        out_specs=pl.BlockSpec(memory_space=pltpu.VMEM),
        scratch_shapes=scratch,
        compiler_params=pltpu.CompilerParams(
            collective_id=0, has_side_effects=True, vmem_limit_bytes=54500 * 1024
        ),
        name="substeps",
    )(*small, pressure, east_wind, north_wind, vertical_wind, sound_squared)


def solution(mesh):
    placed = (
        P("mem", None, "ty", "tx"),
        P("mem", None, "ty", "tx"),
        P("mem", None, "ty", "tx"),
        P("mem", None, "ty", "tx"),
        P(None, "ty", "tx"),
        P(),
        P(),
    )

    def step(*args):
        levels = args[0].shape[1]
        dims = (
            mesh.shape["mem"], mesh.shape["ty"], mesh.shape["tx"], levels,
            args[0].shape[2] , args[0].shape[3], 25 if levels % 25 == 0 else 1,
        )
        return local(dims, *args)

    return jax.shard_map(
        step,
        mesh=mesh,
        in_specs=placed,
        out_specs=P("ty", "tx", None, "mem", None),
        check_vma=False,
    )
```

```python
import functools

import jax
import jax.numpy as jnp
from jax import lax
from jax.experimental import pallas as pl
from jax.experimental.pallas import tpu as pltpu
from jax.sharding import PartitionSpec as P

HR = 0.35
VR = 1.5
PAD = 8
MESH = pl.DeviceIdType.MESH


def kernel(dims, thick_h, owner_h, p_h, ew_h, nw_h, w_h, ss_h, out_ref, *scratch):
    NM, NR, NC, NZ, CY, CX, U = dims
    (
        thick, owner,
        p_v, ew_v, nw_v, w_v, ss_v, part_v, v_v,
        rp_v, g_v, f_v, lam_v, c_v, h_v, hw_v, he_v,
        z_send, srow_p, srow_q, row_p, zh_send, shrow_n, shrow_s, edge_p, edge_n, rrow_n,
        z_w, z_e, rrow_p, rrow_q, zh_w, zh_e, rhrow_s, rhrow_n,
        edge_h, sum_v, acc_v, i_send, i_recv, ce_send, cw_send, ce_recv, cw_recv,
        rn_send, rs_send, rs_recv, rn_recv,
        gath_a, gath_b, send_a, send_b, recv_a, recv_b,
        tok_sem, ld_sem, hs_sem, hr_sem, is_sem, ir_sem, ces_sem, cer_sem, cws_sem, cwr_sem,
        rns_sem, rsr_sem, rss_sem, rnr_sem,
        ga_s, ga_r, gb_s, gb_r, sa_s, sa_r, sb_s, sb_r,
    ) = scratch
    Q = CY // NM
    m = lax.axis_index("mem")
    r = lax.axis_index("ty")
    c = lax.axis_index("tx")

    def mm(d):
        return lax.rem(m + d, NM)

    def rr(d):
        return lax.rem(r + d + NR, NR)

    def cc(d):
        return lax.rem(c + d + NC, NC)

    own = pl.ds(PAD, CY)
    load_p = [pltpu.make_async_copy(p_h.at[a], p_v.at[a, :, own, :], ld_sem.at[a]) for a in range(2)]
    load_e = [pltpu.make_async_copy(ew_h.at[a], ew_v.at[a], ld_sem.at[2 + a]) for a in range(2)]
    load_n = pltpu.make_async_copy(nw_h, nw_v.at[:, :, own, :], ld_sem.at[4])
    load_s = pltpu.make_async_copy(ss_h, ss_v, ld_sem.at[5])
    load_w = pltpu.make_async_copy(w_h, w_v.at[:, pl.ds(1, NZ - 1), :, :], ld_sem.at[6])
    load_t = pltpu.make_async_copy(thick_h, thick, ld_sem.at[7])
    load_o = pltpu.make_async_copy(owner_h, owner, ld_sem.at[8])
    load_rows = [pltpu.make_async_copy(nw_h.at[:, :, 0, :], srow_q, ld_sem.at[9])]
    for ld in (load_s, load_t, load_p[0], load_e[0], *load_rows, load_p[1], load_e[1], load_n, load_w, load_o):
        ld.start()

    barrier = pltpu.get_barrier_semaphore()
    east, west = (m, r, cc(1)), (m, r, cc(-1))
    north, south = (m, rr(1), c), (m, rr(-1), c)
    around = (north, south, east, west)
    peers = [*around, *((mm(d), r, c) for d in range(1, NM))]
    for peer in peers:
        pl.semaphore_signal(barrier, inc=1, device_id=peer, device_id_type=MESH)

    sends = []

    def send(src, dst, ssem, rsem, dev):
        copy = pltpu.make_async_remote_copy(
            src_ref=src, dst_ref=dst, send_sem=ssem, recv_sem=rsem,
            device_id=dev, device_id_type=MESH,
        )
        copy.start()
        sends.append(copy)
        return copy

    def arrived(ref, sem, slot):
        pltpu.make_async_copy(ref.at[slot], ref.at[slot], sem.at[slot]).wait()

    def tell(sem):
        for peer in around:
            pl.semaphore_signal(sem, inc=1, device_id=peer, device_id_type=MESH)

    lane = lax.broadcasted_iota(jnp.int32, (CY, CX), 1)
    row = lax.broadcasted_iota(jnp.int32, (CY, CX), 0)
    lane8 = lax.broadcasted_iota(jnp.int32, (8, CX), 1)
    row8 = lax.broadcasted_iota(jnp.int32, (8, CX), 0)
    zero = jnp.zeros((CY, CX), jnp.float32)
    line = jnp.zeros((1, CX), jnp.float32)

    def blocked(body, init, u=U):
        if u >= NZ:
            for k in range(NZ):
                init = body(k, init)
            return init

        def step(b, carry):
            for j in range(u):
                carry = body(b * u + j, carry)
            return carry

        return lax.fori_loop(0, NZ // u, step, init)

    def pack(a):
        load_p[a].wait()
        load_e[a].wait()

        def body(k, z):
            p = p_v[a, k, own, :]
            edge = jnp.where(lane == CX - 1, p, ew_v[a, k] - HR * p)
            srow_p[a, pl.ds(k, 1), :] = p[CY - 1 : CY]
            row_p[a, pl.ds(k, 1), :] = p[0:1]
            return jnp.where((lane >> 1) == k, pltpu.roll(edge, 2 * k + 1, 1), z)

        z_send[a] = blocked(body, zero, NZ)

    def send_rows(a):
        srow_q[a] = srow_q[a] - HR * row_p[a]
        return [
            send(srow_p.at[a], rrow_p.at[a], hs_sem.at[a], hr_sem.at[a], north),
            send(srow_q.at[a], rrow_q.at[a], hs_sem.at[10 + a], hr_sem.at[10 + a], south),
        ]

    def send_edges(a):
        return [
            send(z_send.at[a], z_w.at[a], hs_sem.at[2 + a], hr_sem.at[2 + a], east),
            send(z_send.at[a], z_e.at[a], hs_sem.at[4 + a], hr_sem.at[4 + a], west),
        ]

    load_s.wait()
    load_t.wait()

    def factor(k, carry):
        b_below, rp_below, ts_below, lv = carry
        ss = ss_v[k]
        b = (VR * VR) * ss
        pivot = (1.0 + b + b_below) - b_below * (b_below * rp_below)
        rp = jnp.where(k > 0, 1.0, 0.0) / pivot
        g = b_below * rp
        ts = thick[k] * ss
        lv = (VR * (ts - ts_below)) * rp + g * lv
        rp_v[k] = rp
        g_v[k] = g
        f_v[k] = b * rp
        lam_v[k] = lv
        return b, rp, ts, lv

    blocked(factor, (zero, zero, zero, zero), NZ)

    pack(0)
    for ld in load_rows:
        ld.wait()
    pl.semaphore_wait(barrier, len(peers))
    halo_rows = send_rows(0)
    halo = send_edges(0)
    tell(tok_sem.at[0])
    pack(1)
    halo_rows += send_rows(1)
    halo += send_edges(1)

    def adjoint(i, carry):
        lam_up, z = carry
        k = NZ - 1 - i
        lam = lam_v[k] + f_v[k] * lam_up
        gg = thick[k] + VR * (lam_up - lam)
        h = gg * ss_v[k]
        lam_v[k] = lam
        c_v[k] = gg - (1.4 * HR) * h
        h_v[k, own, :] = h
        shrow_n[pl.ds(k, 1), :] = h[CY - 1 : CY]
        shrow_s[pl.ds(k, 1), :] = h[0:1]
        return lam, jnp.where((lane >> 1) == k, pltpu.roll(h, 2 * k + 1, 1), z)

    zh_send[...] = blocked(adjoint, (zero, zero), NZ)[1]
    halo += [
        send(shrow_n, rhrow_s, hs_sem.at[6], hr_sem.at[6], north),
        send(shrow_s, rhrow_n, hs_sem.at[7], hr_sem.at[7], south),
        send(zh_send, zh_w, hs_sem.at[8], hr_sem.at[8], east),
        send(zh_send, zh_e, hs_sem.at[9], hr_sem.at[9], west),
    ]
    load_n.wait()

    def clear(k, carry):
        for a in range(2):
            p_v[a, k, pl.ds(PAD - 1, 1), :] = line
            p_v[a, k, pl.ds(PAD + CY, 1), :] = line
            nw_v[a, k, pl.ds(PAD + CY, 1), :] = line
        h_v[k, pl.ds(PAD - 1, 1), :] = line
        h_v[k, pl.ds(PAD + CY, 1), :] = line
        return carry

    blocked(clear, 0)
    small = jnp.zeros((8, CX), jnp.float32)

    def inner(b):
        rows = pl.ds(8 * b, 8)
        here, below, above = (pl.ds(PAD + 8 * b + o, 8) for o in (0, -1, 1))

        def body(k, carry):
            hs = HR * ss_v[k, rows, :]
            h = h_v[k, here, :]
            h_below = h_v[k, below, :]
            hw = pltpu.roll(h, 1, 1)
            hw_v[k, rows, :] = hw
            he_v[k, rows, :] = pltpu.roll(h, CX - 1, 1)
            t = thick[k]
            out = []
            for a in range(2):
                s = carry[a]
                p = p_v[a, k, here, :]
                hp = HR * p
                q = ew_v[a, k, rows, :] - hp
                ew1 = q + pltpu.roll(hp, 1, 1)
                nw1 = (nw_v[a, k, here, :] - hp) + HR * p_v[a, k, below, :]
                ee = hp + pltpu.roll(q, CX - 1, 1)
                nn = (nw_v[a, k, above, :] - HR * p_v[a, k, above, :]) + hp
                part_v[a, k, rows, :] = p - hs * ((ee - ew1) + (nn - nw1))
                out.append((
                    s[0] + t * ew1,
                    s[1] + t * nw1,
                    s[2] + h * (ew1 + nw1),
                    s[3] + hw * ew1,
                    s[4] + h_below * nw1,
                ))
            return tuple(out)

        done = blocked(body, ((small,) * 5,) * 2, NZ)
        for a in range(2):
            for j in range(5):
                sum_v[j, a, rows, :] = done[a][j]

    inner(0)
    inner(1)
    for b in range(2, CY // 8):
        inner(b)

    w_v[:, pl.ds(0, 1), :, :] = jnp.zeros((2, 1, CY, CX), jnp.float32)
    even = (lane & 1) == 0
    odd = (lane & 1) == 1

    def spread(k, t):
        return jnp.where((lane8 >> 1) == k, thick[k], t)

    t_lane = blocked(spread, small, NZ)
    h_first = pltpu.roll(zh_send[...], CX - 1, 1)

    load_w.wait()
    for copy in halo[:4]:
        copy.wait_recv()

    first_lane = lane == 0
    for a in range(2):
        own_z = z_send[a]
        from_w = jnp.where(even, z_w[a] - own_z, 0.0)
        edge_h[a] = jnp.where(even, from_w, pltpu.roll(z_e[a] - own_z, CX - 2, 1))
        z_w[a] = jnp.where(odd, own_z + HR * pltpu.roll(z_w[a], 1, 1), 0.0)
        t_all = jnp.concatenate([t_lane] * (CY // 8), axis=0)
        more_e = HR * jnp.sum(from_w * t_all, axis=1, keepdims=True)
        more_h = HR * jnp.sum(from_w * h_first, axis=1, keepdims=True)
        sum_v[0, a] += jnp.where(first_lane, more_e, 0.0)
        sum_v[2, a] += jnp.where(first_lane, more_h, 0.0)
    div_lane = jnp.where(lane8 == CX - 1, 1.0, jnp.where(lane8 == 0, -HR, 0.0))

    def forward(blocks):
        def body(k, carry):
            out = []
            for i, b in enumerate(blocks):
                rows = pl.ds(8 * b, 8)
                hs = HR * ss_v[k, rows, :]
                rp = rp_v[k, rows, :]
                g = g_v[k, rows, :]
                for a in range(2):
                    part_below, v = carry[2 * i + a]
                    more = pltpu.roll(edge_h[a, rows, :], 2 * CX - 2 * k, 1) * div_lane
                    if b == 0:
                        more = more - jnp.where(row8 == 0, HR * rrow_p[a, pl.ds(k, 1), :], 0.0)
                    if b == CY // 8 - 1:
                        more = more + jnp.where(row8 == 7, rrow_q[a, pl.ds(k, 1), :], 0.0)
                    part = part_v[a, k, rows, :] - hs * more
                    v = (w_v[a, k, rows, :] - VR * (part - part_below)) * rp + g * v
                    part_v[a, k, rows, :] = part
                    v_v[a, k, rows, :] = v
                    out.append((part, v))
            return tuple(out)

        blocked(body, ((small, small),) * (2 * len(blocks)), NZ)

    def backward(blocks):
        pair8 = lane8 >> 1

        def body(i, carry):
            k = NZ - 1 - i
            t = thick[k]
            out = []
            for n, b in enumerate(blocks):
                rows = pl.ds(8 * b, 8)
                f = f_v[k, rows, :]
                lam = lam_v[k, rows, :]
                cc0 = c_v[k, rows, :]
                vs = VR * ss_v[k, rows, :]
                hs = h_v[k, pl.ds(PAD - 1 + 8 * b, 8), :]
                hn = h_v[k, pl.ds(PAD + 1 + 8 * b, 8), :]
                hwk = hw_v[k, rows, :]
                hek = he_v[k, rows, :]
                for a in range(2):
                    w_up, s = carry[2 * n + a]
                    w = v_v[a, k, rows, :] + f * w_up
                    p1 = part_v[a, k, rows, :] - vs * (w_up - w)
                    if b == 0:
                        edge_n[a, pl.ds(k, 1), :] = p1[0:1]
                    if b == CY // 8 - 1:
                        edge_p[a, pl.ds(k, 1), :] = p1[7:8]
                    s = (
                        s[0] + (cc0 * p1 + lam * w),
                        s[1] + hwk * p1,
                        s[2] + hek * p1,
                        s[3] + hs * p1,
                        s[4] + hn * p1,
                        s[5] + t * p1,
                        jnp.where(pair8 == k, pltpu.roll(p1, 2 * k + 1, 1), s[6]),
                    )
                    out.append((w, s))
            return tuple(out)

        done = blocked(body, ((small, (small,) * 7),) * (2 * len(blocks)), NZ)
        for n, b in enumerate(blocks):
            rows = pl.ds(8 * b, 8)
            for a in range(2):
                s = done[2 * n + a][1]
                acc_v[0, a, rows, :] = s[0] + HR * sum_v[2, a, rows, :]
                acc_v[1, a, rows, :] = (HR * HR) * s[1] - HR * sum_v[3, a, rows, :]
                acc_v[2, a, rows, :] = (HR * HR) * s[2]
                acc_v[3, a, rows, :] = (HR * HR) * s[3] - HR * sum_v[4, a, rows, :]
                acc_v[4, a, rows, :] = (HR * HR) * s[4]
                acc_v[5, a, rows, :] = HR * s[5]
                z_e[a, rows, :] = s[6]

    forward(tuple(range(1, CY // 8 - 1)))
    pl.semaphore_wait(tok_sem.at[0], len(around))
    tell(tok_sem.at[1])

    backward(tuple(range(1, CY // 8 - 1)))

    for copy in halo_rows:
        copy.wait_recv()
    t_rows = jnp.concatenate([jnp.full((1, CX), 0.0, jnp.float32) + thick[k] for k in range(NZ)], axis=0)
    for a in range(2):
        below = HR * rrow_p[a]
        sum_v[1, a, pl.ds(0, 1), :] += jnp.sum(below * t_rows, axis=0, keepdims=True)
        sum_v[2, a, pl.ds(0, 1), :] += jnp.sum(below * shrow_s[...], axis=0, keepdims=True)
        rrow_n[a] = srow_q[a] + below
    forward((0, CY // 8 - 1))

    backward((0, CY // 8 - 1))

    rn_send[...] = jnp.zeros_like(rn_send)
    rs_send[...] = jnp.zeros_like(rs_send)
    halo[4].wait_recv()
    halo[5].wait_recv()
    for a in range(2):
        rn_send[a : a + 1, :] = (HR * HR) * jnp.sum(rhrow_n[...] * edge_p[a], axis=0, keepdims=True)
        rn_send[2 + a : 3 + a, :] = acc_v[5, a, pl.ds(CY - 1, 1), :]
        rs_send[a : a + 1, :] = HR * jnp.sum(
            rhrow_s[...] * (HR * edge_n[a] - rrow_n[a]), axis=0, keepdims=True
        )
    send(rn_send, rs_recv.at[m], rns_sem.at[0], rsr_sem.at[m], (0, rr(1), c))
    send(rs_send, rn_recv.at[m], rss_sem.at[0], rnr_sem.at[m], (NM - 1, rr(-1), c))

    halo[6].wait_recv()
    halo[7].wait_recv()

    to_e, to_w = zero, zero
    h_west = pltpu.roll(zh_w[...], 1, 1)
    h_east = pltpu.roll(zh_e[...], CX - 1, 1)
    for a in range(2):
        base, xe, xw, xn, xs, hp = (acc_v[j, a] for j in range(6))
        mass = (
            base
            + jnp.where(lane == CX - 1, 0.0, pltpu.roll(xe, CX - 1, 1))
            + jnp.where(lane == 0, 0.0, pltpu.roll(xw, 1, 1))
            + jnp.where(row == CY - 1, 0.0, pltpu.roll(xn, CY - 1, 0))
            + jnp.where(row == 0, 0.0, pltpu.roll(xs, 1, 0))
        )
        e2 = sum_v[0, a] - (hp - jnp.where(lane == 0, 0.0, pltpu.roll(hp, 1, 1)))
        n2 = sum_v[1, a] - (hp - jnp.where(row == 0, 0.0, pltpu.roll(hp, 1, 0)))
        for q in range(NM):
            i_send[q, 3 * a] = mass[q * Q : (q + 1) * Q]
            i_send[q, 3 * a + 1] = e2[q * Q : (q + 1) * Q]
            i_send[q, 3 * a + 2] = n2[q * Q : (q + 1) * Q]
        ends = z_e[a]
        xw_last = (HR * HR) * jnp.sum(jnp.where(even, h_east * ends, 0.0), axis=1, keepdims=True)
        xe_first = HR * jnp.sum(jnp.where(odd, h_west * (HR * ends - z_w[a]), 0.0), axis=1, keepdims=True)
        to_e = jnp.where(lane == a, xw_last, to_e)
        to_e = jnp.where(lane == 2 + a, pltpu.roll(hp, a + 3, 1), to_e)
        to_w = jnp.where(lane == a, xe_first, to_w)
    for q in range(NM):
        ce_send[q] = to_e[q * Q : (q + 1) * Q]
        cw_send[q] = to_w[q * Q : (q + 1) * Q]

    for d in range(NM):
        q = mm(d)
        send(ce_send.at[q], ce_recv.at[m], ces_sem.at[q], cer_sem.at[m], (q, r, cc(1)))
        send(cw_send.at[q], cw_recv.at[m], cws_sem.at[q], cwr_sem.at[m], (q, r, cc(-1)))
    for d in range(1, NM):
        q = mm(d)
        send(i_send.at[q], i_recv.at[m], is_sem.at[q], ir_sem.at[m], (q, r, c))
    i_recv[m] = i_send[m]
    pl.semaphore_wait(tok_sem.at[1], len(around))
    tell(tok_sem.at[2])

    for d in range(1, NM):
        arrived(i_recv, ir_sem, mm(d))
    for d in range(NM):
        arrived(ce_recv, cer_sem, mm(d))
        arrived(cw_recv, cwr_sem, mm(d))

    @pl.when(m == 0)
    def _():
        for d in range(NM):
            arrived(rs_recv, rsr_sem, mm(d))
        for s in range(NM):
            for a in range(2):
                i_recv[s, 3 * a, 0:1, :] += rs_recv[s, a : a + 1, :]
                i_recv[s, 3 * a + 2, 0:1, :] += rs_recv[s, 2 + a : 3 + a, :]

    @pl.when(m == NM - 1)
    def _():
        for d in range(NM):
            arrived(rn_recv, rnr_sem, mm(d))
        for s in range(NM):
            for a in range(2):
                i_recv[s, 3 * a, Q - 1 : Q, :] += rn_recv[s, a : a + 1, :]

    members = 2 * NM
    fields = ([], [], [])
    for s in range(NM):
        ce = ce_recv[s]
        cw = cw_recv[s]
        for a in range(2):
            mass = i_recv[s, 3 * a]
            mass += jnp.where(lane8 == 0, pltpu.roll(ce, CX - a, 1) if a else ce, 0.0)
            mass += jnp.where(lane8 == CX - 1, pltpu.roll(cw, CX - 1 - a, 1), 0.0)
            e2 = i_recv[s, 3 * a + 1]
            e2 += jnp.where(lane8 == 0, pltpu.roll(ce, CX - 2 - a, 1), 0.0)
            fields[0].append(mass)
            fields[1].append(e2)
            fields[2].append(i_recv[s, 3 * a + 2])
    for j in range(3):
        mean = sum(fields[j][1:], fields[j][0]) * (1.0 / members)
        devs = [(x - mean) * (x - mean) for x in fields[j]]
        gath_a[c, j] = mean
        gath_b[r, j] = sum(devs[1:], devs[0]) * (1.0 / (members - 1))

    def far(n):
        return sorted(range(1, n), key=lambda d: -min(d, n - d))

    pl.semaphore_wait(tok_sem.at[2], len(around))
    for d in far(NC):
        send(gath_a.at[c], gath_a.at[c], ga_s.at[d], ga_r.at[c], (m, r, cc(d)))
    for d in far(NR):
        send(gath_b.at[r], gath_b.at[r], gb_s.at[d], gb_r.at[r], (m, rr(d), c))

    load_o.wait()
    wanted = [rr(d) * NC + c for d in range(NR)] + [r * NC + cc(d) for d in range(1, NC)]

    def find(i, got):
        for j in range(8 if NR * NC % 8 == 0 else 1):
            t = i * (8 if NR * NC % 8 == 0 else 1) + j
            o = owner[t]
            got = tuple(jnp.where(o == w, t, g) for w, g in zip(wanted, got))
        return got

    steps = NR * NC // 8 if NR * NC % 8 == 0 else NR * NC
    source = lax.fori_loop(0, steps, find, tuple(jnp.int32(0) for _ in wanted))
    col_source, row_source = source[:NR], source[:1] + source[NR:]

    for d in range(1, NC):
        arrived(gath_a, ga_r, cc(d))
    for d in far(NR):
        send_a[d] = gath_a[lax.rem(col_source[d], NC)]
        send(send_a.at[d], recv_a.at[r], sa_s.at[d], sa_r.at[r], (m, rr(d), c))
    for d in range(1, NR):
        arrived(gath_b, gb_r, rr(d))
    for d in far(NC):
        send_b[d] = gath_b[row_source[d] // NC]
        send(send_b.at[d], recv_b.at[c], sb_s.at[d], sb_r.at[c], (m, r, cc(d)))
    recv_a[r] = gath_a[lax.rem(source[0], NC)]
    recv_b[c] = gath_b[source[0] // NC]
    for d in range(1, NR):
        arrived(recv_a, sa_r, rr(d))
    for d in range(1, NC):
        arrived(recv_b, sb_r, cc(d))
    out_ref[0, 0, 0:3] = recv_a[source[0] // NC]
    out_ref[0, 0, 3:6] = recv_b[lax.rem(source[0], NC)]
    for copy in sends:
        copy.wait_send()


def local(dims, pressure, east_wind, north_wind, vertical_wind, sound_squared, thickness, owner_map):
    NM, NR, NC, NZ, CY, CX, U = dims
    Q = CY // NM
    f32 = jnp.float32
    V = pltpu.VMEM
    D = pltpu.SemaphoreType.DMA
    rows = CY + 2 * PAD
    two = (2, NZ, CY, CX)
    one = (NZ, CY, CX)
    tile = (CY, CX)
    pair = (2, CY, CX)
    scratch = [
        pltpu.SMEM((NZ,), f32), pltpu.SMEM((NR * NC,), jnp.int32),
        V((2, NZ, rows, CX), f32), V(two, f32), V((2, NZ, rows, CX), f32), V(two, f32), V(one, f32),
        V(two, f32), V(two, f32),
        V(one, f32), V(one, f32), V(one, f32), V(one, f32), V(one, f32),
        V((NZ, rows, CX), f32), V(one, f32), V(one, f32),
        V(pair, f32), V((2, NZ, CX), f32), V((2, NZ, CX), f32), V((2, NZ, CX), f32),
        V(tile, f32), V((NZ, CX), f32), V((NZ, CX), f32),
        V((2, NZ, CX), f32), V((2, NZ, CX), f32), V((2, NZ, CX), f32),
        V(pair, f32), V(pair, f32), V((2, NZ, CX), f32), V((2, NZ, CX), f32),
        V(tile, f32), V(tile, f32), V((NZ, CX), f32), V((NZ, CX), f32),
        V(pair, f32), V((5, 2, CY, CX), f32), V((6, 2, CY, CX), f32), V((NM, 6, Q, CX), f32), V((NM, 6, Q, CX), f32),
        V((NM, Q, CX), f32), V((NM, Q, CX), f32), V((NM, Q, CX), f32), V((NM, Q, CX), f32),
        V((8, CX), f32), V((8, CX), f32), V((NM, 8, CX), f32), V((NM, 8, CX), f32),
        V((NC, 3, Q, CX), f32), V((NR, 3, Q, CX), f32),
        V((NR, 3, Q, CX), f32), V((NC, 3, Q, CX), f32),
        V((NR, 3, Q, CX), f32), V((NC, 3, Q, CX), f32),
        pltpu.SemaphoreType.REGULAR((3,)), D((10,)), D((12,)), D((12,)), D((NM,)), D((NM,)),
        D((NM,)), D((NM,)), D((NM,)), D((NM,)),
        D((1,)), D((NM,)), D((1,)), D((NM,)),
        D((NC,)), D((NC,)), D((NR,)), D((NR,)), D((NR,)), D((NR,)), D((NC,)), D((NC,)),
    ]
    hbm = pl.BlockSpec(memory_space=pl.ANY)
    small = [pltpu.with_memory_space_constraint(x, pltpu.HBM) for x in (thickness, owner_map)]
    return pl.pallas_call(
        functools.partial(kernel, dims),
        out_shape=jax.ShapeDtypeStruct((1, 1, 6, Q, CX), f32),
        in_specs=[hbm] * 7,
        out_specs=pl.BlockSpec(memory_space=pltpu.VMEM),
        scratch_shapes=scratch,
        compiler_params=pltpu.CompilerParams(
            collective_id=0, has_side_effects=True, vmem_limit_bytes=54500 * 1024
        ),
        name="substeps",
    )(*small, pressure, east_wind, north_wind, vertical_wind, sound_squared)


def solution(mesh):
    placed = (
        P("mem", None, "ty", "tx"),
        P("mem", None, "ty", "tx"),
        P("mem", None, "ty", "tx"),
        P("mem", None, "ty", "tx"),
        P(None, "ty", "tx"),
        P(),
        P(),
    )

    def step(*args):
        levels = args[0].shape[1]
        dims = (
            mesh.shape["mem"], mesh.shape["ty"], mesh.shape["tx"], levels,
            args[0].shape[2] , args[0].shape[3], 25 if levels % 25 == 0 else 1,
        )
        return local(dims, *args)

    return jax.shard_map(
        step,
        mesh=mesh,
        in_specs=placed,
        out_specs=P("ty", "tx", None, "mem", None),
        check_vma=False,
    )
```

```python
import functools

import jax
import jax.numpy as jnp
from jax import lax
from jax.experimental import pallas as pl
from jax.experimental.pallas import tpu as pltpu
from jax.sharding import PartitionSpec as P

HR = 0.35
VR = 1.5
PAD = 8
MESH = pl.DeviceIdType.MESH


def kernel(dims, thick_h, owner_h, p_h, ew_h, nw_h, w_h, ss_h, out_ref, *scratch):
    NM, NR, NC, NZ, CY, CX, U = dims
    (
        thick, owner,
        p_v, ew_v, nw_v, w_v, ss_v, part_v, v_v,
        rp_v, g_v, f_v, lam_v, c_v, h_v, hw_v, he_v,
        z_send, srow_p, srow_q, row_p, zh_send, shrow_n, shrow_s, edge_p, edge_n, rrow_n,
        z_w, z_e, rrow_p, rrow_q, zh_w, zh_e, rhrow_s, rhrow_n,
        edge_h, sum_v, acc_v, i_send, i_recv, ce_send, cw_send, ce_recv, cw_recv,
        rn_send, rs_send, rs_recv, rn_recv,
        gath_a, gath_b, send_a, send_b, recv_a, recv_b,
        tok_sem, ld_sem, hs_sem, hr_sem, is_sem, ir_sem, ces_sem, cer_sem, cws_sem, cwr_sem,
        rns_sem, rsr_sem, rss_sem, rnr_sem,
        ga_s, ga_r, gb_s, gb_r, sa_s, sa_r, sb_s, sb_r,
    ) = scratch
    Q = CY // NM
    m = lax.axis_index("mem")
    r = lax.axis_index("ty")
    c = lax.axis_index("tx")

    def mm(d):
        return lax.rem(m + d, NM)

    def rr(d):
        return lax.rem(r + d + NR, NR)

    def cc(d):
        return lax.rem(c + d + NC, NC)

    own = pl.ds(PAD, CY)
    load_p = [pltpu.make_async_copy(p_h.at[a], p_v.at[a, :, own, :], ld_sem.at[a]) for a in range(2)]
    load_e = [pltpu.make_async_copy(ew_h.at[a], ew_v.at[a], ld_sem.at[2 + a]) for a in range(2)]
    load_n = pltpu.make_async_copy(nw_h, nw_v.at[:, :, own, :], ld_sem.at[4])
    load_s = pltpu.make_async_copy(ss_h, ss_v, ld_sem.at[5])
    load_w = pltpu.make_async_copy(w_h, w_v.at[:, pl.ds(1, NZ - 1), :, :], ld_sem.at[6])
    load_t = pltpu.make_async_copy(thick_h, thick, ld_sem.at[7])
    load_o = pltpu.make_async_copy(owner_h, owner, ld_sem.at[8])
    load_rows = [pltpu.make_async_copy(nw_h.at[:, :, 0, :], srow_q, ld_sem.at[9])]
    for ld in (load_s, load_t, load_p[0], load_e[0], *load_rows, load_p[1], load_e[1], load_n, load_w, load_o):
        ld.start()

    barrier = pltpu.get_barrier_semaphore()
    east, west = (m, r, cc(1)), (m, r, cc(-1))
    north, south = (m, rr(1), c), (m, rr(-1), c)
    around = (north, south, east, west)
    peers = [*around, *((mm(d), r, c) for d in range(1, NM))]
    for peer in peers:
        pl.semaphore_signal(barrier, inc=1, device_id=peer, device_id_type=MESH)

    sends = []

    def send(src, dst, ssem, rsem, dev):
        copy = pltpu.make_async_remote_copy(
            src_ref=src, dst_ref=dst, send_sem=ssem, recv_sem=rsem,
            device_id=dev, device_id_type=MESH,
        )
        copy.start()
        sends.append(copy)
        return copy

    def arrived(ref, sem, slot):
        pltpu.make_async_copy(ref.at[slot], ref.at[slot], sem.at[slot]).wait()

    def tell(sem):
        for peer in around:
            pl.semaphore_signal(sem, inc=1, device_id=peer, device_id_type=MESH)

    lane = lax.broadcasted_iota(jnp.int32, (CY, CX), 1)
    row = lax.broadcasted_iota(jnp.int32, (CY, CX), 0)
    lane8 = lax.broadcasted_iota(jnp.int32, (8, CX), 1)
    row8 = lax.broadcasted_iota(jnp.int32, (8, CX), 0)
    zero = jnp.zeros((CY, CX), jnp.float32)
    line = jnp.zeros((1, CX), jnp.float32)

    def blocked(body, init, u=U):
        if u >= NZ:
            for k in range(NZ):
                init = body(k, init)
            return init

        def step(b, carry):
            for j in range(u):
                carry = body(b * u + j, carry)
            return carry

        return lax.fori_loop(0, NZ // u, step, init)

    def pack(a):
        load_p[a].wait()
        load_e[a].wait()

        def body(k, z):
            p = p_v[a, k, own, :]
            edge = jnp.where(lane == CX - 1, p, ew_v[a, k] - HR * p)
            srow_p[a, pl.ds(k, 1), :] = p[CY - 1 : CY]
            row_p[a, pl.ds(k, 1), :] = p[0:1]
            return jnp.where((lane >> 1) == k, pltpu.roll(edge, 2 * k + 1, 1), z)

        z_send[a] = blocked(body, zero, NZ)

    def send_rows(a):
        srow_q[a] = srow_q[a] - HR * row_p[a]
        return [
            send(srow_p.at[a], rrow_p.at[a], hs_sem.at[a], hr_sem.at[a], north),
            send(srow_q.at[a], rrow_q.at[a], hs_sem.at[10 + a], hr_sem.at[10 + a], south),
        ]

    def send_edges(a):
        return [
            send(z_send.at[a], z_w.at[a], hs_sem.at[2 + a], hr_sem.at[2 + a], east),
            send(z_send.at[a], z_e.at[a], hs_sem.at[4 + a], hr_sem.at[4 + a], west),
        ]

    load_s.wait()
    load_t.wait()

    def factor(k, carry):
        b_below, rp_below, ts_below, lv = carry
        ss = ss_v[k]
        b = (VR * VR) * ss
        pivot = (1.0 + b + b_below) - b_below * (b_below * rp_below)
        rp = jnp.where(k > 0, 1.0, 0.0) / pivot
        g = b_below * rp
        ts = thick[k] * ss
        lv = (VR * (ts - ts_below)) * rp + g * lv
        rp_v[k] = rp
        g_v[k] = g
        f_v[k] = b * rp
        lam_v[k] = lv
        return b, rp, ts, lv

    blocked(factor, (zero, zero, zero, zero), NZ)

    pack(0)
    for ld in load_rows:
        ld.wait()
    pl.semaphore_wait(barrier, len(peers))
    halo_rows = send_rows(0)
    halo = send_edges(0)
    tell(tok_sem.at[0])
    pack(1)
    halo_rows += send_rows(1)
    halo += send_edges(1)

    def adjoint(i, carry):
        lam_up, z = carry
        k = NZ - 1 - i
        lam = lam_v[k] + f_v[k] * lam_up
        gg = thick[k] + VR * (lam_up - lam)
        h = gg * ss_v[k]
        lam_v[k] = lam
        c_v[k] = gg - (1.4 * HR) * h
        h_v[k, own, :] = h
        shrow_n[pl.ds(k, 1), :] = h[CY - 1 : CY]
        shrow_s[pl.ds(k, 1), :] = h[0:1]
        return lam, jnp.where((lane >> 1) == k, pltpu.roll(h, 2 * k + 1, 1), z)

    zh_send[...] = blocked(adjoint, (zero, zero), NZ)[1]
    halo += [
        send(shrow_n, rhrow_s, hs_sem.at[6], hr_sem.at[6], north),
        send(shrow_s, rhrow_n, hs_sem.at[7], hr_sem.at[7], south),
        send(zh_send, zh_w, hs_sem.at[8], hr_sem.at[8], east),
        send(zh_send, zh_e, hs_sem.at[9], hr_sem.at[9], west),
    ]
    load_n.wait()

    def clear(k, carry):
        for a in range(2):
            p_v[a, k, pl.ds(PAD - 1, 1), :] = line
            p_v[a, k, pl.ds(PAD + CY, 1), :] = line
            nw_v[a, k, pl.ds(PAD + CY, 1), :] = line
        h_v[k, pl.ds(PAD - 1, 1), :] = line
        h_v[k, pl.ds(PAD + CY, 1), :] = line
        return carry

    blocked(clear, 0)
    small = jnp.zeros((8, CX), jnp.float32)

    def inner(b):
        rows = pl.ds(8 * b, 8)
        here, below, above = (pl.ds(PAD + 8 * b + o, 8) for o in (0, -1, 1))

        def body(k, carry):
            hs = HR * ss_v[k, rows, :]
            h = h_v[k, here, :]
            h_below = h_v[k, below, :]
            hw = pltpu.roll(h, 1, 1)
            hw_v[k, rows, :] = hw
            he_v[k, rows, :] = pltpu.roll(h, CX - 1, 1)
            t = thick[k]
            out = []
            for a in range(2):
                s = carry[a]
                p = p_v[a, k, here, :]
                hp = HR * p
                q = ew_v[a, k, rows, :] - hp
                ew1 = q + pltpu.roll(hp, 1, 1)
                nw1 = (nw_v[a, k, here, :] - hp) + HR * p_v[a, k, below, :]
                ee = hp + pltpu.roll(q, CX - 1, 1)
                nn = (nw_v[a, k, above, :] - HR * p_v[a, k, above, :]) + hp
                part_v[a, k, rows, :] = p - hs * ((ee - ew1) + (nn - nw1))
                out.append((
                    s[0] + t * ew1,
                    s[1] + t * nw1,
                    s[2] + h * (ew1 + nw1),
                    s[3] + hw * ew1,
                    s[4] + h_below * nw1,
                ))
            return tuple(out)

        done = blocked(body, ((small,) * 5,) * 2, NZ)
        for a in range(2):
            for j in range(5):
                sum_v[j, a, rows, :] = done[a][j]

    inner(0)
    inner(1)
    for b in range(2, CY // 8):
        inner(b)

    w_v[:, pl.ds(0, 1), :, :] = jnp.zeros((2, 1, CY, CX), jnp.float32)
    even = (lane & 1) == 0
    odd = (lane & 1) == 1

    def spread(k, t):
        return jnp.where((lane8 >> 1) == k, thick[k], t)

    t_lane = blocked(spread, small, NZ)
    h_first = pltpu.roll(zh_send[...], CX - 1, 1)

    load_w.wait()
    for copy in halo[:4]:
        copy.wait_recv()

    first_lane = lane == 0
    for a in range(2):
        own_z = z_send[a]
        from_w = jnp.where(even, z_w[a] - own_z, 0.0)
        edge_h[a] = jnp.where(even, from_w, pltpu.roll(z_e[a] - own_z, CX - 2, 1))
        z_w[a] = jnp.where(odd, own_z + HR * pltpu.roll(z_w[a], 1, 1), 0.0)
        t_all = jnp.concatenate([t_lane] * (CY // 8), axis=0)
        more_e = HR * jnp.sum(from_w * t_all, axis=1, keepdims=True)
        more_h = HR * jnp.sum(from_w * h_first, axis=1, keepdims=True)
        sum_v[0, a] += jnp.where(first_lane, more_e, 0.0)
        sum_v[2, a] += jnp.where(first_lane, more_h, 0.0)
    div_lane = jnp.where(lane8 == CX - 1, 1.0, jnp.where(lane8 == 0, -HR, 0.0))

    def forward(blocks):
        def body(k, carry):
            out = []
            for i, b in enumerate(blocks):
                rows = pl.ds(8 * b, 8)
                hs = HR * ss_v[k, rows, :]
                rp = rp_v[k, rows, :]
                g = g_v[k, rows, :]
                for a in range(2):
                    part_below, v = carry[2 * i + a]
                    more = pltpu.roll(edge_h[a, rows, :], 2 * CX - 2 * k, 1) * div_lane
                    if b == 0:
                        more = more - jnp.where(row8 == 0, HR * rrow_p[a, pl.ds(k, 1), :], 0.0)
                    if b == CY // 8 - 1:
                        more = more + jnp.where(row8 == 7, rrow_q[a, pl.ds(k, 1), :], 0.0)
                    part = part_v[a, k, rows, :] - hs * more
                    v = (w_v[a, k, rows, :] - VR * (part - part_below)) * rp + g * v
                    part_v[a, k, rows, :] = part
                    v_v[a, k, rows, :] = v
                    out.append((part, v))
            return tuple(out)

        blocked(body, ((small, small),) * (2 * len(blocks)), NZ)

    def backward(blocks):
        pair8 = lane8 >> 1

        def body(i, carry):
            k = NZ - 1 - i
            t = thick[k]
            out = []
            for n, b in enumerate(blocks):
                rows = pl.ds(8 * b, 8)
                f = f_v[k, rows, :]
                lam = lam_v[k, rows, :]
                cc0 = c_v[k, rows, :]
                vs = VR * ss_v[k, rows, :]
                hs = h_v[k, pl.ds(PAD - 1 + 8 * b, 8), :]
                hn = h_v[k, pl.ds(PAD + 1 + 8 * b, 8), :]
                hwk = hw_v[k, rows, :]
                hek = he_v[k, rows, :]
                for a in range(2):
                    w_up, s = carry[2 * n + a]
                    w = v_v[a, k, rows, :] + f * w_up
                    p1 = part_v[a, k, rows, :] - vs * (w_up - w)
                    if b == 0:
                        edge_n[a, pl.ds(k, 1), :] = p1[0:1]
                    if b == CY // 8 - 1:
                        edge_p[a, pl.ds(k, 1), :] = p1[7:8]
                    s = (
                        s[0] + (cc0 * p1 + lam * w),
                        s[1] + hwk * p1,
                        s[2] + hek * p1,
                        s[3] + hs * p1,
                        s[4] + hn * p1,
                        s[5] + t * p1,
                        jnp.where(pair8 == k, pltpu.roll(p1, 2 * k + 1, 1), s[6]),
                    )
                    out.append((w, s))
            return tuple(out)

        done = blocked(body, ((small, (small,) * 7),) * (2 * len(blocks)), NZ)
        for n, b in enumerate(blocks):
            rows = pl.ds(8 * b, 8)
            for a in range(2):
                s = done[2 * n + a][1]
                acc_v[0, a, rows, :] = s[0] + HR * sum_v[2, a, rows, :]
                acc_v[1, a, rows, :] = (HR * HR) * s[1] - HR * sum_v[3, a, rows, :]
                acc_v[2, a, rows, :] = (HR * HR) * s[2]
                acc_v[3, a, rows, :] = (HR * HR) * s[3] - HR * sum_v[4, a, rows, :]
                acc_v[4, a, rows, :] = (HR * HR) * s[4]
                acc_v[5, a, rows, :] = HR * s[5]
                z_e[a, rows, :] = s[6]

    forward(tuple(range(1, CY // 8 - 1)))
    pl.semaphore_wait(tok_sem.at[0], len(around))
    tell(tok_sem.at[1])

    backward(tuple(range(1, CY // 8 - 1)))

    for copy in halo_rows:
        copy.wait_recv()
    t_rows = jnp.concatenate([jnp.full((1, CX), 0.0, jnp.float32) + thick[k] for k in range(NZ)], axis=0)
    for a in range(2):
        below = HR * rrow_p[a]
        sum_v[1, a, pl.ds(0, 1), :] += jnp.sum(below * t_rows, axis=0, keepdims=True)
        sum_v[2, a, pl.ds(0, 1), :] += jnp.sum(below * shrow_s[...], axis=0, keepdims=True)
        rrow_n[a] = srow_q[a] + below
    forward((0, CY // 8 - 1))

    backward((0, CY // 8 - 1))

    rn_send[...] = jnp.zeros_like(rn_send)
    rs_send[...] = jnp.zeros_like(rs_send)
    halo[4].wait_recv()
    halo[5].wait_recv()
    for a in range(2):
        rn_send[a : a + 1, :] = (HR * HR) * jnp.sum(rhrow_n[...] * edge_p[a], axis=0, keepdims=True)
        rn_send[2 + a : 3 + a, :] = acc_v[5, a, pl.ds(CY - 1, 1), :]
        rs_send[a : a + 1, :] = HR * jnp.sum(
            rhrow_s[...] * (HR * edge_n[a] - rrow_n[a]), axis=0, keepdims=True
        )
    send(rn_send, rs_recv.at[m], rns_sem.at[0], rsr_sem.at[m], (0, rr(1), c))
    send(rs_send, rn_recv.at[m], rss_sem.at[0], rnr_sem.at[m], (NM - 1, rr(-1), c))

    halo[6].wait_recv()
    halo[7].wait_recv()

    to_e, to_w = zero, zero
    h_west = pltpu.roll(zh_w[...], 1, 1)
    h_east = pltpu.roll(zh_e[...], CX - 1, 1)
    for a in range(2):
        base, xe, xw, xn, xs, hp = (acc_v[j, a] for j in range(6))
        mass = (
            base
            + jnp.where(lane == CX - 1, 0.0, pltpu.roll(xe, CX - 1, 1))
            + jnp.where(lane == 0, 0.0, pltpu.roll(xw, 1, 1))
            + jnp.where(row == CY - 1, 0.0, pltpu.roll(xn, CY - 1, 0))
            + jnp.where(row == 0, 0.0, pltpu.roll(xs, 1, 0))
        )
        e2 = sum_v[0, a] - (hp - jnp.where(lane == 0, 0.0, pltpu.roll(hp, 1, 1)))
        n2 = sum_v[1, a] - (hp - jnp.where(row == 0, 0.0, pltpu.roll(hp, 1, 0)))
        for q in range(NM):
            i_send[q, 3 * a] = mass[q * Q : (q + 1) * Q]
            i_send[q, 3 * a + 1] = e2[q * Q : (q + 1) * Q]
            i_send[q, 3 * a + 2] = n2[q * Q : (q + 1) * Q]
        ends = z_e[a]
        xw_last = (HR * HR) * jnp.sum(jnp.where(even, h_east * ends, 0.0), axis=1, keepdims=True)
        xe_first = HR * jnp.sum(jnp.where(odd, h_west * (HR * ends - z_w[a]), 0.0), axis=1, keepdims=True)
        hp_last = jnp.sum(jnp.where(lane == CX - 1, hp, 0.0), axis=1, keepdims=True)
        to_e = jnp.where(lane == Q * a + (row & (Q - 1)), xw_last, to_e)
        to_e = jnp.where(lane == Q * (2 + a) + (row & (Q - 1)), hp_last, to_e)
        to_w = jnp.where(lane == Q * a + (row & (Q - 1)), xe_first, to_w)
    for q in range(NM):
        ce_send[q] = jnp.sum(to_e[q * Q : (q + 1) * Q], axis=0, keepdims=True)
        cw_send[q] = jnp.sum(to_w[q * Q : (q + 1) * Q], axis=0, keepdims=True)

    for d in (*range(1, NM), 0):
        q = mm(d)
        send(ce_send.at[q], ce_recv.at[m], ces_sem.at[q], cer_sem.at[m], (q, r, cc(1)))
        send(cw_send.at[q], cw_recv.at[m], cws_sem.at[q], cwr_sem.at[m], (q, r, cc(-1)))
    for d in range(1, NM):
        q = mm(d)
        send(i_send.at[q], i_recv.at[m], is_sem.at[q], ir_sem.at[m], (q, r, c))
    i_recv[m] = i_send[m]
    pl.semaphore_wait(tok_sem.at[1], len(around))
    tell(tok_sem.at[2])

    for d in range(1, NM):
        arrived(i_recv, ir_sem, mm(d))
    for d in range(NM):
        arrived(ce_recv, cer_sem, mm(d))
        arrived(cw_recv, cwr_sem, mm(d))

    @pl.when(m == 0)
    def _():
        for d in range(NM):
            arrived(rs_recv, rsr_sem, mm(d))
        for s in range(NM):
            for a in range(2):
                i_recv[s, 3 * a, 0:1, :] += rs_recv[s, a : a + 1, :]
                i_recv[s, 3 * a + 2, 0:1, :] += rs_recv[s, 2 + a : 3 + a, :]

    @pl.when(m == NM - 1)
    def _():
        for d in range(NM):
            arrived(rn_recv, rnr_sem, mm(d))
        for s in range(NM):
            for a in range(2):
                i_recv[s, 3 * a, Q - 1 : Q, :] += rn_recv[s, a : a + 1, :]

    members = 2 * NM

    def upright(x, j):
        return jnp.sum(jnp.where(lane8 == Q * j + row8, x, 0.0), axis=1, keepdims=True)

    fields = ([], [], [])
    for s in range(NM):
        ce = jnp.broadcast_to(ce_recv[s], (Q, CX))
        cw = jnp.broadcast_to(cw_recv[s], (Q, CX))
        for a in range(2):
            mass = i_recv[s, 3 * a]
            mass += jnp.where(lane8 == 0, upright(ce, a), jnp.where(lane8 == CX - 1, upright(cw, a), 0.0))
            e2 = i_recv[s, 3 * a + 1]
            e2 += jnp.where(lane8 == 0, upright(ce, 2 + a), 0.0)
            fields[0].append(mass)
            fields[1].append(e2)
            fields[2].append(i_recv[s, 3 * a + 2])
    for j in range(3):
        mean = sum(fields[j][1:], fields[j][0]) * (1.0 / members)
        devs = [(x - mean) * (x - mean) for x in fields[j]]
        gath_a[c, j] = mean
        gath_b[r, j] = sum(devs[1:], devs[0]) * (1.0 / (members - 1))

    def far(n):
        return sorted(range(1, n), key=lambda d: -min(d, n - d))

    pl.semaphore_wait(tok_sem.at[2], len(around))
    for d in far(NC):
        send(gath_a.at[c], gath_a.at[c], ga_s.at[d], ga_r.at[c], (m, r, cc(d)))
    for d in far(NR):
        send(gath_b.at[r], gath_b.at[r], gb_s.at[d], gb_r.at[r], (m, rr(d), c))

    load_o.wait()
    wanted = [rr(d) * NC + c for d in range(NR)] + [r * NC + cc(d) for d in range(1, NC)]

    def find(i, got):
        for j in range(8 if NR * NC % 8 == 0 else 1):
            t = i * (8 if NR * NC % 8 == 0 else 1) + j
            o = owner[t]
            got = tuple(jnp.where(o == w, t, g) for w, g in zip(wanted, got))
        return got

    steps = NR * NC // 8 if NR * NC % 8 == 0 else NR * NC
    source = lax.fori_loop(0, steps, find, tuple(jnp.int32(0) for _ in wanted))
    col_source, row_source = source[:NR], source[:1] + source[NR:]

    for d in range(1, NC):
        arrived(gath_a, ga_r, cc(d))
    for d in far(NR):
        send_a[d] = gath_a[lax.rem(col_source[d], NC)]
        send(send_a.at[d], recv_a.at[r], sa_s.at[d], sa_r.at[r], (m, rr(d), c))
    for d in range(1, NR):
        arrived(gath_b, gb_r, rr(d))
    for d in far(NC):
        send_b[d] = gath_b[row_source[d] // NC]
        send(send_b.at[d], recv_b.at[c], sb_s.at[d], sb_r.at[c], (m, r, cc(d)))
    recv_a[r] = gath_a[lax.rem(source[0], NC)]
    recv_b[c] = gath_b[source[0] // NC]
    for d in range(1, NR):
        arrived(recv_a, sa_r, rr(d))
    for d in range(1, NC):
        arrived(recv_b, sb_r, cc(d))
    out_ref[0, 0, 0:3] = recv_a[source[0] // NC]
    out_ref[0, 0, 3:6] = recv_b[lax.rem(source[0], NC)]
    for copy in sends:
        copy.wait_send()


def local(dims, pressure, east_wind, north_wind, vertical_wind, sound_squared, thickness, owner_map):
    NM, NR, NC, NZ, CY, CX, U = dims
    Q = CY // NM
    f32 = jnp.float32
    V = pltpu.VMEM
    D = pltpu.SemaphoreType.DMA
    rows = CY + 2 * PAD
    two = (2, NZ, CY, CX)
    one = (NZ, CY, CX)
    tile = (CY, CX)
    pair = (2, CY, CX)
    scratch = [
        pltpu.SMEM((NZ,), f32), pltpu.SMEM((NR * NC,), jnp.int32),
        V((2, NZ, rows, CX), f32), V(two, f32), V((2, NZ, rows, CX), f32), V(two, f32), V(one, f32),
        V(two, f32), V(two, f32),
        V(one, f32), V(one, f32), V(one, f32), V(one, f32), V(one, f32),
        V((NZ, rows, CX), f32), V(one, f32), V(one, f32),
        V(pair, f32), V((2, NZ, CX), f32), V((2, NZ, CX), f32), V((2, NZ, CX), f32),
        V(tile, f32), V((NZ, CX), f32), V((NZ, CX), f32),
        V((2, NZ, CX), f32), V((2, NZ, CX), f32), V((2, NZ, CX), f32),
        V(pair, f32), V(pair, f32), V((2, NZ, CX), f32), V((2, NZ, CX), f32),
        V(tile, f32), V(tile, f32), V((NZ, CX), f32), V((NZ, CX), f32),
        V(pair, f32), V((5, 2, CY, CX), f32), V((6, 2, CY, CX), f32), V((NM, 6, Q, CX), f32), V((NM, 6, Q, CX), f32),
        V((NM, 1, CX), f32), V((NM, 1, CX), f32), V((NM, 1, CX), f32), V((NM, 1, CX), f32),
        V((8, CX), f32), V((8, CX), f32), V((NM, 8, CX), f32), V((NM, 8, CX), f32),
        V((NC, 3, Q, CX), f32), V((NR, 3, Q, CX), f32),
        V((NR, 3, Q, CX), f32), V((NC, 3, Q, CX), f32),
        V((NR, 3, Q, CX), f32), V((NC, 3, Q, CX), f32),
        pltpu.SemaphoreType.REGULAR((3,)), D((10,)), D((12,)), D((12,)), D((NM,)), D((NM,)),
        D((NM,)), D((NM,)), D((NM,)), D((NM,)),
        D((1,)), D((NM,)), D((1,)), D((NM,)),
        D((NC,)), D((NC,)), D((NR,)), D((NR,)), D((NR,)), D((NR,)), D((NC,)), D((NC,)),
    ]
    hbm = pl.BlockSpec(memory_space=pl.ANY)
    small = [pltpu.with_memory_space_constraint(x, pltpu.HBM) for x in (thickness, owner_map)]
    return pl.pallas_call(
        functools.partial(kernel, dims),
        out_shape=jax.ShapeDtypeStruct((1, 1, 6, Q, CX), f32),
        in_specs=[hbm] * 7,
        out_specs=pl.BlockSpec(memory_space=pltpu.VMEM),
        scratch_shapes=scratch,
        compiler_params=pltpu.CompilerParams(
            collective_id=0, has_side_effects=True, vmem_limit_bytes=54500 * 1024
        ),
        name="substeps",
    )(*small, pressure, east_wind, north_wind, vertical_wind, sound_squared)


def solution(mesh):
    placed = (
        P("mem", None, "ty", "tx"),
        P("mem", None, "ty", "tx"),
        P("mem", None, "ty", "tx"),
        P("mem", None, "ty", "tx"),
        P(None, "ty", "tx"),
        P(),
        P(),
    )

    def step(*args):
        levels = args[0].shape[1]
        dims = (
            mesh.shape["mem"], mesh.shape["ty"], mesh.shape["tx"], levels,
            args[0].shape[2] , args[0].shape[3], 25 if levels % 25 == 0 else 1,
        )
        return local(dims, *args)

    return jax.shard_map(
        step,
        mesh=mesh,
        in_specs=placed,
        out_specs=P("ty", "tx", None, "mem", None),
        check_vma=False,
    )
```
